128 devices in a mesh: bx: 4 (over z_hi, core), by: 8 (over z_lo, x), bz: 4 (over y).
Axes of the slice: x: 4, y: 4, z: 4 (z_hi: 2, z_lo: 2; z = z_hi * 2 + z_lo), core: 2. Of those that a mesh axis runs over, the one named last changes fastest.
Arguments:
- estimate: float32 [64, 128, 512], P('bx', 'by', 'bz'), may hold values from 0.2 to 5
- observed: float32 [8, 64, 128, 512], P(None, 'bx', 'by', 'bz'), may hold values from 0.3 to 180, as said below
- coverage: int32 [8, 4, 8, 4], P(None, 'bx', 'by', 'bz'), may hold values from 0 to 1, as said below
- psf_taps: float32 [8, 3, 17], replicated, may hold values from 0.05 to 1
Outputs:
- refined: float32 [64, 128, 512], P('bx', 'by', 'bz')
The draws below stay inside these ranges and needn't reach their ends.
Inputs may be any that keep to these rules, and one draw needn't show every extreme that they name: `coverage`: each block is covered by 2 to 8 views; in every draw some block is covered by all 8. `observed`: positive.
All inputs are finite; a program needn't handle non-finite values.
Results may differ from the reference program's by a relative error of at most 0.0001.
Values sent between devices are 32-bit elements; how exact they have to be, the bound alone decides.
No kernel may reach another device: no remote copies, remote signals or barrier semaphores. Data moves between devices by JAX's collectives and lax.ppermute only.
A program may use at most 64 MiB of HBM per device.

```python
import math
import jax
import jax.numpy as jnp
from jax import lax

V = 8
R = 8
CX = 16
CY = 16
CZ = 128
NX = 64
NY = 128
NZ = 512
N_BX = 4
N_BY = 8
N_BZ = 4


def draw_observed(key, part):
    first, second = jax.random.split(key, 2)
    blocks_x = NX // CX
    blocks_y = NY // CY
    blocks_z = NZ // CZ
    coarse = jnp.exp(jax.random.uniform(first, (blocks_x, blocks_y, blocks_z), jnp.float32, 0.0, jnp.log(10.0)))
    ramp = 1.0 + 2.0 * jnp.arange(blocks_y, dtype=jnp.float32) / max(blocks_y - 1, 1)
    coarse = coarse * ramp[None, :, None]
    grown = jnp.repeat(jnp.repeat(jnp.repeat(coarse, CX, axis=0), CY, axis=1), CZ, axis=2)
    voxel = jnp.exp(jax.random.uniform(second, (V, NX, NY, NZ), jnp.float32, jnp.log(0.3), jnp.log(3.0)))
    values = voxel * grown[None]
    return values.astype(jnp.float32)


def draw_coverage(key, part):
    blocks = NX // CX * (NY // CY) * (NZ // CZ)
    first, second, third = jax.random.split(jax.random.fold_in(key, 7), 3)
    counts = jax.random.randint(first, (blocks,), 2, V + 1)
    fullest = jax.random.randint(second, (), 0, blocks)
    counts = counts.at[fullest].set(V)
    ranks = jax.vmap(lambda each: jax.random.permutation(each, V))(jax.random.split(third, blocks))
    covered = (ranks < counts[:, None]).astype(jnp.int32)
    return covered.T.reshape(V, NX // CX, NY // CY, NZ // CZ)


def levels(key, dims, cuts, least, high):
    def one(position, shards_of):
        steps = jax.random.uniform(jax.random.fold_in(jax.random.fold_in(key, 6), position), (shards_of,), jnp.float32, least / len(cuts), high / len(cuts))
        return jnp.repeat(jnp.exp(steps), dims[position] // shards_of).reshape((-1,) + (1,) * (len(dims) - position - 1))

    factor_of = one(*cuts[0])
    for cut in cuts[1:]:
        factor_of = factor_of * one(*cut)
    return factor_of


def setup_inputs(seed: int = 0) -> dict:
    key_list = jax.random.split(jax.random.key(seed), 5)
    return {
        "estimate": jnp.clip(jnp.exp(math.log(5.0) - 3.218876 * jax.random.uniform(key_list[0], (NX, NY, NZ), jnp.float32) ** levels(key_list[0], (NX, NY, NZ), ((0, 4), (1, 8), (2, 4)), -0.2, 0.2)), 0.2, 5.0),
        "observed": draw_observed(jax.random.fold_in(key_list[4], 71), 0),
        "coverage": draw_coverage(jax.random.fold_in(key_list[4], 71), 0),
        "psf_taps": jnp.clip(jnp.exp(jax.random.uniform(key_list[3], (V, 3, 2 * R + 1), jnp.float32, math.log(0.05), math.log(1.0))), 0.05, 1.0),
    }


def blur_axis(field, taps_row, axis):
    moved = jnp.moveaxis(field, axis, -1)
    shape = moved.shape
    flat = moved.reshape(-1, 1, shape[-1])
    kernel = taps_row.reshape(1, 1, -1)
    width = (taps_row.shape[0] - 1) // 2
    result = lax.conv_general_dilated(flat, kernel, (1,), [(width, width)], precision=lax.Precision.HIGHEST)
    return jnp.moveaxis(result.reshape(shape), -1, axis)


def blur_volume(field, kernels):
    result = field
    for axis in range(3):
        result = blur_axis(result, kernels[axis], axis)
    return result


def spread(block_values):
    grown = jnp.broadcast_to(block_values[:, None, :, None, :, None], (N_BX, CX, N_BY, CY, N_BZ, CZ))
    return grown.reshape(NX, NY, NZ)


def reference(estimate, observed, coverage, psf_taps):
    taps = psf_taps / jnp.sum(psf_taps, axis=2, keepdims=True)
    weights = coverage.astype(jnp.float32)
    count = spread(jnp.sum(weights, axis=0))
    summed = jnp.zeros((NX, NY, NZ), jnp.float32)
    target_field = jnp.zeros((NX, NY, NZ), jnp.float32)
    for view in range(V):
        blurred = blur_volume(estimate, taps[view])
        ratio = observed[view] / blurred
        back = blur_volume(ratio, taps[view][:, ::-1])
        weight_full = spread(weights[view])
        summed = summed + weight_full * back
        target_field = target_field + weight_full * observed[view]
    updated = estimate * (summed / count)
    target = jnp.sum(target_field / count)
    total = jnp.sum(updated)
    return updated * (target / total)
```

```python
import jax
import jax.numpy as jnp
from jax import lax
from jax.sharding import PartitionSpec as P

ALL = ("bx", "by", "bz")
HIGH = lax.Precision.HIGH


def swap(low, high, axis):
    count = lax.axis_size(axis)
    odd = lax.axis_index(axis) % 2 == 1

    def pairs(first):
        both = []
        for i in range(first, count - 1, 2):
            both += [(i, i + 1), (i + 1, i)]
        return both

    one = lax.ppermute(jnp.where(odd, low, high), axis, pairs(0))
    two = lax.ppermute(jnp.where(odd, high, low), axis, pairs(1))
    return jnp.where(odd, one, two), jnp.where(odd, two, one)


def band_matrices(taps, n_out):
    length = taps.shape[1]
    n_in = n_out + length - 1
    offset = jnp.arange(n_in)[:, None] - jnp.arange(n_out)[None, :]
    select = offset[:, :, None] == jnp.arange(length)
    return jnp.sum(jnp.where(select[None], taps[:, None, None, :], 0.0), axis=3)


def spread(blocks, shape, radius):
    for dim, size in enumerate(shape):
        sizes = (radius, size - 2 * radius, radius)
        parts = []
        for k in range(3):
            part = lax.slice_in_dim(blocks, k, k + 1, axis=dim + 1)
            full = part.shape[: dim + 1] + (sizes[k],) + part.shape[dim + 2 :]
            parts.append(jnp.broadcast_to(part, full))
        blocks = jnp.concatenate(parts, axis=dim + 1)
    return blocks


def on_device(estimate, observed, coverage, psf_taps):
    views = observed.shape[0]
    radius = (psf_taps.shape[2] - 1) // 2
    size_x, size_y, size_z = estimate.shape
    taps = psf_taps / jnp.sum(psf_taps, axis=2, keepdims=True)
    weights = coverage.reshape(views).astype(jnp.float32)
    count = jnp.sum(weights)
    target_local = jnp.sum(weights * jnp.sum(observed, axis=(1, 2, 3))) / count

    field = estimate
    blocks = weights.reshape(views, 1, 1, 1)
    for dim, axis in enumerate(ALL):
        low = lax.slice_in_dim(field, 0, radius, axis=dim)
        high = lax.slice_in_dim(field, field.shape[dim] - radius, field.shape[dim], axis=dim)
        flat = blocks.reshape(-1)
        below, above = swap(
            jnp.concatenate([low.reshape(-1), flat]), jnp.concatenate([high.reshape(-1), flat]), axis
        )
        cells = low.size
        field = jnp.concatenate(
            [below[:cells].reshape(low.shape), field, above[:cells].reshape(high.shape)], axis=dim
        )
        blocks = jnp.concatenate(
            [below[cells:].reshape(blocks.shape), blocks, above[cells:].reshape(blocks.shape)],
            axis=dim + 1,
        )

    band_x = band_matrices(taps[:, 0], size_x)
    band_y = band_matrices(taps[:, 1], size_y)
    band_z = band_matrices(taps[:, 2], size_z)
    section = jnp.einsum("xyz,vzc->vxyc", field, band_z, precision=HIGH)
    section = jnp.einsum("vxyc,vyb->vxbc", section, band_y, precision=HIGH)
    blurred = jnp.einsum("vxbc,vxa->vabc", section, band_x, precision=HIGH)
    ratio = observed / blurred
    back = jnp.einsum("vabc,vxa->vxbc", ratio, band_x, precision=HIGH)
    back = jnp.einsum("vxbc,vyb->vxyc", back, band_y, precision=HIGH)
    back = jnp.einsum("vxyc,vzc->vxyz", back, band_z, precision=HIGH)
    part = jnp.sum(spread(blocks, field.shape, radius) * back, axis=0)
    counts = jnp.maximum(jnp.sum(blocks, axis=0), 1.0)
    total_local = jnp.sum(field * part / spread(counts[None], field.shape, radius)[0])

    both = jnp.concatenate([jnp.full((64,), target_local), jnp.full((64,), total_local)])
    peers = lax.axis_size(ALL)
    gathered = lax.all_to_all(jnp.broadcast_to(both[None], (peers, 128)), ALL, 0, 0)
    sums = jnp.sum(gathered, axis=0)
    target, total = sums[0], sums[64]

    for dim, axis in reversed(tuple(enumerate(ALL))):
        inner = part.shape[dim] - radius
        low = lax.slice_in_dim(part, 0, radius, axis=dim)
        high = lax.slice_in_dim(part, inner, part.shape[dim], axis=dim)
        below, above = swap(low, high, axis)
        mine = lax.slice_in_dim(part, radius, inner, axis=dim)
        gap = list(mine.shape)
        gap[dim] -= 2 * radius
        added = jnp.concatenate([below, jnp.zeros(gap, jnp.float32), above], axis=dim)
        part = mine + added
    updated = estimate * (part / count)
    return updated * (target / total)


def solution(mesh):
    spec = P("bx", "by", "bz")
    views_spec = P(None, "bx", "by", "bz")
    return jax.shard_map(
        on_device,
        mesh=mesh,
        in_specs=(spec, views_spec, views_spec, P()),
        out_specs=spec,
        check_vma=False,
    )
```

```python
import jax
import jax.numpy as jnp
from jax import lax
from jax.experimental import pallas as pl
from jax.experimental.pallas import tpu as pltpu
from jax.sharding import PartitionSpec as P

ALL = ("bx", "by", "bz")
F32, BF16 = jnp.float32, jnp.bfloat16
V, R, K = 8, 8, 17
CX, CY, CZ = 16, 16, 128
EX, EY = CX + 2 * R, CY + 2 * R
ROWS = EX * EY
LANES = 128


def pairs(count, first):
    both = []
    for i in range(first, count - 1, 2):
        both += [(i, i + 1), (i + 1, i)]
    return both


def swap(one, two, axis):
    count = lax.axis_size(axis)
    return lax.ppermute(one, axis, pairs(count, 0)), lax.ppermute(two, axis, pairs(count, 1))


def kernel_call(body, out_shape, scratch=(), in_smem=0, flops=0, n_in=0):
    vmem = pl.BlockSpec(memory_space=pltpu.VMEM)
    smem = pl.BlockSpec(memory_space=pltpu.SMEM)
    return pl.pallas_call(
        body,
        out_shape=out_shape,
        in_specs=[smem] * in_smem + [vmem] * (n_in - in_smem),
        out_specs=jax.tree.map(lambda _: vmem, out_shape),
        scratch_shapes=list(scratch),
        compiler_params=pltpu.CompilerParams(vmem_limit_bytes=48 * 1024 * 1024),
        cost_estimate=pl.CostEstimate(flops=flops, bytes_accessed=1024, transcendentals=0),
    )


def shape(*dims, dtype=F32):
    return jax.ShapeDtypeStruct(dims, dtype)


def x_pack(flag, est, w, op1, op2):
    odd = flag[0] == 1
    for a in range(R):
        low, high = est[a], est[CX - R + a]
        op1[a * CY : (a + 1) * CY, :] = jnp.where(odd, low, high)
        op2[a * CY : (a + 1) * CY, :] = jnp.where(odd, high, low)
    op1[R * CY :, :] = w[...]
    op2[R * CY :, :] = w[...]


def y_pack(flag, est, w, x1, x2, field, ws, op1, op2):
    odd_x, odd_y = flag[0] == 1, flag[1] == 1
    one, two = x1[...], x2[...]
    below, above = jnp.where(odd_x, one, two), jnp.where(odd_x, two, one)
    cells = R * CY
    field[:R] = below[:cells].reshape(R, CY, LANES)
    field[R : R + CX] = est[...]
    field[R + CX :] = above[:cells].reshape(R, CY, LANES)
    ws[:V] = below[cells:]
    ws[V : 2 * V] = w[...]
    ws[2 * V :] = above[cells:]
    for i in range(EX):
        low, high = field[i, :R], field[i, CY - R :]
        op1[i * R : (i + 1) * R, :] = jnp.where(odd_y, low, high)
        op2[i * R : (i + 1) * R, :] = jnp.where(odd_y, high, low)
    op1[EX * R :, :] = ws[...]
    op2[EX * R :, :] = ws[...]


def z_pack(flag, fx, wx, y1, y2, field, ws, op1, op2):
    odd_y, odd_z = flag[1] == 1, flag[2] == 1
    one, two = y1[...], y2[...]
    below, above = jnp.where(odd_y, one, two), jnp.where(odd_y, two, one)
    cells = EX * R
    field[:, :R] = below[:cells].reshape(EX, R, LANES)
    field[:, R : R + CY] = fx[...]
    field[:, R + CY :] = above[:cells].reshape(EX, R, LANES)
    ws[: 3 * V] = below[cells:]
    ws[3 * V : 6 * V] = wx[...]
    ws[6 * V :] = above[cells:]
    turned = jnp.transpose(field[...].reshape(ROWS, LANES))
    low, high = turned[:R], turned[CZ - R :]
    op1[:, :ROWS] = jnp.where(odd_z, low, high)
    op2[:, :ROWS] = jnp.where(odd_z, high, low)
    for b in range(9):
        part = ws[b * V : (b + 1) * V]
        op1[:, ROWS + b * LANES : ROWS + (b + 1) * LANES] = part
        op2[:, ROWS + b * LANES : ROWS + (b + 1) * LANES] = part


def total_of(x):
    return jnp.sum(jnp.sum(x, axis=0, keepdims=True), axis=1, keepdims=True)


def split(x):
    high = x.astype(BF16)
    return high, (x - high.astype(F32)).astype(BF16)


def main_kernel(
    flag, taps, field, w9, z1, z2, observed, wz1, wz2, tz1, tz2,
    part, op1, op2, sums,
    ab, eb, hs, tx, rp, uy, ub, edge, edges, ws,
):
    odd_z = flag[2] == 1
    one, two = z1[...], z2[...]
    below, above = jnp.where(odd_z, one, two), jnp.where(odd_z, two, one)
    for b in range(9):
        ws[b * V : (b + 1) * V] = below[:, ROWS + b * LANES : ROWS + (b + 1) * LANES]
        ws[(18 + b) * V : (19 + b) * V] = above[:, ROWS + b * LANES : ROWS + (b + 1) * LANES]
    ws[9 * V : 18 * V] = w9[...]

    edges[:R] = below[:, :ROWS]
    edges[R:] = above[:, :ROWS]
    e = edges[...]
    e_high = e.astype(BF16).astype(F32)
    e_low = e - e_high
    stacked = jnp.concatenate([e_high, e_low, e_high, jnp.zeros((LANES - 6 * R, ROWS), F32)], axis=0)
    eb[...] = jnp.transpose(stacked).astype(BF16)

    for c in range(4):
        rows = slice(c * 256, (c + 1) * 256)
        high, low = split(field[c * 8 : (c + 1) * 8].reshape(256, LANES))
        ab[rows, :LANES] = high
        ab[rows, LANES:] = low
    for c in range(4):
        rows = slice(c * 256, (c + 1) * 256)
        first = ab[rows, :]
        second = jnp.concatenate([ab[rows, :LANES], eb[rows, :]], axis=1)
        for n in range(4):
            cols = slice(n * 256, (n + 1) * 256)
            got = jnp.dot(first, wz1[:, cols], preferred_element_type=F32)
            got += jnp.dot(second, wz2[:, cols], preferred_element_type=F32)
            hs[2 * n, c * 8 : (c + 1) * 8] = got[:, :LANES].reshape(8, EY, LANES)
            hs[2 * n + 1, c * 8 : (c + 1) * 8] = got[:, LANES:].reshape(8, EY, LANES)

    rp[...] = jnp.zeros_like(rp)
    part[...] = jnp.zeros_like(part)
    edge[...] = jnp.zeros_like(edge)
    lane = lax.broadcasted_iota(jnp.int32, (8, LANES), 1)

    def view_step(v, seen):
        t = [[taps[(v * 3 + d) * K + k] for k in range(K)] for d in range(2)]
        for y in range(EY // 8):
            rows = slice(y * 8, (y + 1) * 8)
            for a in range(CX):
                acc = t[0][0] * hs[v, a, rows]
                for k in range(1, K):
                    acc += t[0][k] * hs[v, a + k, rows]
                tx[a, rows] = acc
        own = ws[pl.ds(13 * V + v, 1), :]
        for a in range(CX):
            for b in range(CY // 8):
                acc = t[1][0] * tx[a, b * 8 : b * 8 + 8]
                for k in range(1, K):
                    acc += t[1][k] * tx[a, b * 8 + k : b * 8 + k + 8]
                seen_here = observed[v, a, b * 8 : b * 8 + 8]
                seen = seen + own * seen_here
                rp[a, 16 + b * 8 : 24 + b * 8] = seen_here / acc
        for a in range(CX):
            for m in range(EY // 8):
                acc = None
                for k in range(K):
                    start = 16 + 8 * m - k
                    if start + 8 <= 16 or start >= 32:
                        continue
                    term = t[1][k] * rp[a, start : start + 8]
                    acc = term if acc is None else acc + term
                uy[a, m * 8 : m * 8 + 8] = acc
        for y in range(EY // 16):
            rows = slice(y * 16, (y + 1) * 16)
            for i in range(EX):
                acc = None
                for a in range(max(0, i - K + 1), min(CX, i + 1)):
                    term = t[0][i - a] * uy[a, rows]
                    acc = term if acc is None else acc + term
                high, low = split(acc)
                ub[i * EY + y * 16 : i * EY + (y + 1) * 16, :LANES] = high
                ub[i * EY + y * 16 : i * EY + (y + 1) * 16, LANES:] = low
        for c in range(4):
            rows = slice(c * 256, (c + 1) * 256)
            got = jnp.dot(ub[rows, :], tz1[v], preferred_element_type=F32)
            got += jnp.dot(ub[rows, :LANES], tz2[v], preferred_element_type=F32)
            bx = (0, 1, 1, 2)[c]
            for j in range(3):
                ys = ((0, 8), (8, 24), (24, 32))[j]
                here = slice(ys[0], ys[1])
                at = j * 3 + bx
                w_mid = ws[pl.ds((9 + at) * V + v, 1), :]
                w_edge = jnp.where(
                    lane < R, ws[pl.ds(at * V + v, 1), :], ws[pl.ds((18 + at) * V + v, 1), :]
                )[:1]
                for i in range(8):
                    r0 = i * EY
                    part[c * 8 + i, here] += w_mid * got[r0 + ys[0] : r0 + ys[1], :LANES]
                    edge[c * 256 + r0 + ys[0] : c * 256 + r0 + ys[1], :] += (
                        w_edge * got[r0 + ys[0] : r0 + ys[1], LANES:]
                    )
        return seen

    seen = lax.fori_loop(0, V, view_step, jnp.zeros((8, LANES), F32))

    turned = jnp.transpose(edge[...])
    low, high = turned[:R], turned[R : 2 * R]
    op1[...] = jnp.where(odd_z, low, high)
    op2[...] = jnp.where(odd_z, high, low)

    def count_of(block):
        return jnp.maximum(
            jnp.sum(ws[block * V : (block + 1) * V], axis=0, keepdims=True), 1.0
        )

    total = jnp.zeros((8, LANES), F32)
    place = lax.broadcasted_iota(jnp.int32, (8, ROWS), 1)
    in_y = place % EY
    y_band = jnp.where(in_y < R, 0, jnp.where(in_y < R + CY, 1, 2))
    low_sum = edges[:R] * low
    high_sum = edges[R:] * high
    for bx in range(3):
        xs = ((0, 8), (8, 24), (24, 32))[bx]
        for j in range(3):
            ys = ((0, 8), (8, 24), (24, 32))[j]
            at = j * 3 + bx
            block = field[xs[0] : xs[1], ys[0] : ys[1]] * part[xs[0] : xs[1], ys[0] : ys[1]]
            block = block.reshape((-1, 8, LANES))
            total += jnp.sum(block, axis=0) / count_of(9 + at)
            lanes = slice(xs[0] * EY, xs[1] * EY)
            picked = y_band[:, lanes] == j
            for side, first in ((low_sum, 0), (high_sum, 18)):
                cut = jnp.where(picked, side[:, lanes], 0.0)
                folded = cut[:, :LANES]
                for q in range(1, cut.shape[1] // LANES):
                    folded = folded + cut[:, q * LANES : (q + 1) * LANES]
                total += folded / count_of(first + at)
    target = seen / count_of(13)
    both = jnp.where(lane < 64, total_of(target), total_of(total))
    for p in range(sums.shape[0]):
        sums[p] = both


def z_add(flag, part, r1, r2, mid, op1, op2):
    odd_y, odd_z = flag[1] == 1, flag[2] == 1
    one, two = r1[...], r2[...]
    below, above = jnp.where(odd_z, one, two), jnp.where(odd_z, two, one)
    stacked = jnp.concatenate([below, jnp.zeros((CZ - 2 * R, ROWS), F32), above], axis=0)
    added = jnp.transpose(stacked).reshape(EX, EY, LANES)
    for i in range(EX):
        plane = part[i] + added[i]
        mid[i] = plane[R : R + CY]
        low, high = plane[:R], plane[R + CY :]
        op1[i * R : (i + 1) * R, :] = jnp.where(odd_y, low, high)
        op2[i * R : (i + 1) * R, :] = jnp.where(odd_y, high, low)


def y_add(flag, part, r1, r2, mid, op1, op2):
    odd_x, odd_y = flag[0] == 1, flag[1] == 1
    for i in range(EX):
        one, two = r1[i * R : (i + 1) * R], r2[i * R : (i + 1) * R]
        first = part[i, :R] + jnp.where(odd_y, one, two)
        second = part[i, R:] + jnp.where(odd_y, two, one)
        if i < R:
            at = i
            rows = slice(at * CY, at * CY + R), slice(at * CY + R, (at + 1) * CY)
            op2[rows[0], :] = first
            op2[rows[1], :] = second
        elif i < R + CX:
            mid[i - R, :R] = first
            mid[i - R, R:] = second
        else:
            at = i - R - CX
            rows = slice(at * CY, at * CY + R), slice(at * CY + R, (at + 1) * CY)
            for row, new in zip(rows, (first, second)):
                low = op2[row, :]
                op1[row, :] = jnp.where(odd_x, low, new)
                op2[row, :] = jnp.where(odd_x, new, low)


def x_add(flag, part, r1, r2, est, count, sums, out):
    odd_x = flag[0] == 1
    gathered = jnp.sum(sums[...], axis=0)[:1]
    lane = lax.broadcasted_iota(jnp.int32, (1, LANES), 1)
    target = jnp.sum(jnp.where(lane == 0, gathered, 0.0), axis=1, keepdims=True)
    total = jnp.sum(jnp.where(lane == 64, gathered, 0.0), axis=1, keepdims=True)
    scale = target / total
    counts = jnp.sum(count[...], axis=0, keepdims=True)
    for a in range(CX):
        rows = slice((a % R) * CY, (a % R + 1) * CY)
        one, two = r1[rows, :], r2[rows, :]
        got = jnp.where(odd_x, one, two) if a < R else jnp.where(odd_x, two, one)
        out[a] = est[a] * ((part[a] + got) / counts) * scale


def z_bands(taps):
    near = jnp.arange(CZ + 2 * R)
    offset = near[:, None] - jnp.arange(CZ)[None, :]
    picked = offset[None, :, :, None] == jnp.arange(K)
    band = jnp.sum(jnp.where(picked, taps[:, None, None, :], 0.0), axis=3)
    high = lax.reduce_precision(band, 8, 7)
    low = band - high
    pad = jnp.zeros((V, LANES - 6 * R, CZ), F32)

    def faces(x):
        return jnp.concatenate([x[:, :R], x[:, R + CZ :]], axis=1)

    def middle(x):
        return x[:, R : R + CZ]

    wz1 = jnp.concatenate([middle(high), middle(high)], axis=1)
    wz2 = jnp.concatenate([middle(low), faces(high), faces(high), faces(low), pad], axis=1)

    def flat(x):
        return jnp.transpose(x, (1, 0, 2)).reshape(2 * LANES, V * CZ).astype(BF16)

    pad2 = jnp.zeros((V, LANES - 2 * R, CZ), F32)

    def turned(x):
        return jnp.transpose(jnp.concatenate([middle(x), faces(x), pad2], axis=1), (0, 2, 1))

    tz1 = jnp.concatenate([turned(high), turned(high)], axis=1).astype(BF16)
    tz2 = turned(low).astype(BF16)
    return flat(wz1), flat(wz2), tz1, tz2


def on_device(estimate, observed, coverage, psf_taps):
    taps = psf_taps / jnp.sum(psf_taps, axis=2, keepdims=True)
    flag = jnp.stack([lax.axis_index(axis) % 2 for axis in ALL]).astype(jnp.int32)
    w = jnp.broadcast_to(coverage.reshape(V, 1).astype(F32), (V, LANES))
    peers = lax.axis_size(ALL)

    op = shape((R * CY) + V, LANES)
    x1, x2 = kernel_call(x_pack, (op, op), n_in=3, in_smem=1)(flag, estimate, w)
    x1, x2 = swap(x1, x2, "bx")
    bands = z_bands(taps[:, 2])
    op = shape(EX * R + 3 * V, LANES)
    fx, wx, y1, y2 = kernel_call(
        y_pack, (shape(EX, CY, LANES), shape(3 * V, LANES), op, op), n_in=5, in_smem=1
    )(flag, estimate, w, x1, x2)
    y1, y2 = swap(y1, y2, "by")
    op = shape(R, ROWS + 9 * LANES)
    field, w9, z1, z2 = kernel_call(
        z_pack, (shape(EX, EY, LANES), shape(9 * V, LANES), op, op), n_in=5, in_smem=1
    )(flag, fx, wx, y1, y2)
    z1, z2 = swap(z1, z2, "bz")

    face = shape(R, ROWS)
    part, z1, z2, sums = kernel_call(
        main_kernel,
        (shape(EX, EY, LANES), face, face, shape(peers, 8, LANES)),
        scratch=(
            pltpu.VMEM((ROWS, 2 * LANES), BF16),
            pltpu.VMEM((ROWS, LANES), BF16),
            pltpu.VMEM((V, EX, EY, LANES), F32),
            pltpu.VMEM((CX, EY, LANES), F32),
            pltpu.VMEM((CX, 48, LANES), F32),
            pltpu.VMEM((CX, EY, LANES), F32),
            pltpu.VMEM((ROWS, 2 * LANES), BF16),
            pltpu.VMEM((ROWS, LANES), F32),
            pltpu.VMEM((2 * R, ROWS), F32),
            pltpu.VMEM((27 * V, LANES), F32),
        ),
        n_in=11,
        in_smem=2,
        flops=2 * 10**9,
    )(flag, taps.reshape(-1), field, w9, z1, z2, observed, *bands)

    sums = lax.all_to_all(sums, ALL, 0, 0)
    z1, z2 = swap(z1, z2, "bz")
    op = shape(EX * R, LANES)
    part, y1, y2 = kernel_call(z_add, (shape(EX, CY, LANES), op, op), n_in=4, in_smem=1)(
        flag, part, z1, z2
    )
    y1, y2 = swap(y1, y2, "by")
    op = shape(R * CY, LANES)
    part, x1, x2 = kernel_call(y_add, (shape(CX, CY, LANES), op, op), n_in=4, in_smem=1)(
        flag, part, y1, y2
    )
    x1, x2 = swap(x1, x2, "bx")
    return kernel_call(x_add, shape(CX, CY, LANES), n_in=7, in_smem=1)(
        flag, part, x1, x2, estimate, w, sums
    )


def solution(mesh):
    spec = P("bx", "by", "bz")
    views_spec = P(None, "bx", "by", "bz")
    return jax.shard_map(
        on_device,
        mesh=mesh,
        in_specs=(spec, views_spec, views_spec, P()),
        out_specs=spec,
        check_vma=False,
    )
```

```python
import jax
import jax.numpy as jnp
from jax import lax
from jax.experimental import pallas as pl
from jax.experimental.pallas import tpu as pltpu
from jax.sharding import PartitionSpec as P

ALL = ("bx", "by", "bz")
F32, BF16 = jnp.float32, jnp.bfloat16
V, R, K = 8, 8, 17
CX, CY, CZ = 16, 16, 128
EX, EY = CX + 2 * R, CY + 2 * R
ROWS = EX * EY
LANES = 128


def pairs(count, first):
    both = []
    for i in range(first, count - 1, 2):
        both += [(i, i + 1), (i + 1, i)]
    return both


def swap(one, two, axis):
    count = lax.axis_size(axis)
    return lax.ppermute(one, axis, pairs(count, 0)), lax.ppermute(two, axis, pairs(count, 1))


def kernel_call(body, out_shape, scratch=(), in_smem=0, flops=0, n_in=0):
    vmem = pl.BlockSpec(memory_space=pltpu.VMEM)
    smem = pl.BlockSpec(memory_space=pltpu.SMEM)
    return pl.pallas_call(
        body,
        out_shape=out_shape,
        in_specs=[smem] * in_smem + [vmem] * (n_in - in_smem),
        out_specs=jax.tree.map(lambda _: vmem, out_shape),
        scratch_shapes=list(scratch),
        compiler_params=pltpu.CompilerParams(vmem_limit_bytes=48 * 1024 * 1024),
        cost_estimate=pl.CostEstimate(flops=flops, bytes_accessed=1024, transcendentals=0),
    )


def shape(*dims, dtype=F32):
    return jax.ShapeDtypeStruct(dims, dtype)


def x_pack(flag, est, w, op1, op2):
    odd = flag[0] == 1
    for a in range(R):
        low, high = est[a], est[CX - R + a]
        op1[a * CY : (a + 1) * CY, :] = jnp.where(odd, low, high)
        op2[a * CY : (a + 1) * CY, :] = jnp.where(odd, high, low)
    op1[R * CY :, :] = w[...]
    op2[R * CY :, :] = w[...]


def y_pack(flag, est, w, x1, x2, field, ws, op1, op2):
    odd_x, odd_y = flag[0] == 1, flag[1] == 1
    one, two = x1[...], x2[...]
    below, above = jnp.where(odd_x, one, two), jnp.where(odd_x, two, one)
    cells = R * CY
    field[:R] = below[:cells].reshape(R, CY, LANES)
    field[R : R + CX] = est[...]
    field[R + CX :] = above[:cells].reshape(R, CY, LANES)
    ws[...] = w[...]
    ws[:1] = below[cells : cells + 1]
    ws[1:2] = w[:1]
    ws[2:3] = above[cells : cells + 1]
    for i in range(EX):
        low, high = field[i, :R], field[i, CY - R :]
        op1[i * R : (i + 1) * R, :] = jnp.where(odd_y, low, high)
        op2[i * R : (i + 1) * R, :] = jnp.where(odd_y, high, low)
    op1[EX * R :, :] = ws[...]
    op2[EX * R :, :] = ws[...]


def z_pack(flag, fx, wx, y1, y2, field, ws, op1, op2):
    odd_y, odd_z = flag[1] == 1, flag[2] == 1
    one, two = y1[...], y2[...]
    below, above = jnp.where(odd_y, one, two), jnp.where(odd_y, two, one)
    cells = EX * R
    field[:, :R] = below[:cells].reshape(EX, R, LANES)
    field[:, R : R + CY] = fx[...]
    field[:, R + CY :] = above[:cells].reshape(EX, R, LANES)
    ws[...] = jnp.zeros_like(ws)
    ws[:3] = below[cells : cells + 3]
    ws[3:6] = wx[:3]
    ws[6:9] = above[cells : cells + 3]
    turned = jnp.transpose(field[...].reshape(ROWS, LANES))
    low, high = turned[:R], turned[CZ - R :]
    op1[:, :ROWS] = jnp.where(odd_z, low, high)
    op2[:, :ROWS] = jnp.where(odd_z, high, low)
    for b in range(2):
        cols = slice(ROWS + b * LANES, ROWS + (b + 1) * LANES)
        op1[:, cols] = ws[b * 8 : b * 8 + 8]
        op2[:, cols] = ws[b * 8 : b * 8 + 8]


def total_of(x):
    return jnp.sum(jnp.sum(x, axis=0, keepdims=True), axis=1, keepdims=True)


def split(x):
    high = x.astype(BF16)
    return high, (x - high.astype(F32)).astype(BF16)


def iota(dims, axis):
    return lax.broadcasted_iota(jnp.int32, dims, axis)


def pick(taps, base, offset):
    got = jnp.zeros(offset.shape, F32)
    for k in range(K):
        got = jnp.where(offset == k, taps[base + k], got)
    return got


def bands(taps, by, byt, wz1, wz2, tz1, tz2):
    for v in range(V):
        base = (v * 3 + 1) * K
        rows = slice(v * CY, (v + 1) * CY)
        column = iota((CY, LANES), 1)
        got = pick(taps, base, column % EY - iota((CY, LANES), 0))
        high, low = split(got)
        by[rows, :] = jnp.where(column < 2 * EY, high.astype(F32), low.astype(F32)).astype(BF16)

    def turned_y(v, got):
        lane = iota((EY, LANES), 1)
        here = pick(taps, (v * 3 + 1) * K, iota((EY, LANES), 0) - lane % CY)
        return jnp.where(lane // CY == v, here, got)

    both = lax.fori_loop(0, V, turned_y, jnp.zeros((EY, LANES), F32))
    high, low = split(both)
    byt[:EY, :] = high.astype(F32)
    byt[EY:, :] = low.astype(F32)

    def z_of(v, carry):
        base = (v * 3 + 2) * K
        row, col = iota((LANES, LANES), 0), iota((LANES, LANES), 1)
        high, low = split(pick(taps, base, row + R - col))
        wz1[v, :LANES, :] = high
        wz1[v, LANES:, :] = high
        wz2[v, :LANES, :] = low
        place = row[: 6 * R] % (2 * R)
        near = jnp.where(place < R, place, place + CZ)
        got = pick(taps, base, near - col[: 6 * R])
        high, low = split(got)
        which = row[: 6 * R] < 4 * R
        wz2[v, LANES : LANES + 6 * R, :] = jnp.where(
            which, high.astype(F32), low.astype(F32)
        ).astype(BF16)
        wz2[v, LANES + 6 * R :, :] = jnp.zeros((LANES - 6 * R, LANES), BF16)
        high, low = split(pick(taps, base, col + R - row))
        tz1[v, :LANES, :LANES] = high
        tz1[v, LANES:, :LANES] = high
        tz2[v, :, :LANES] = low
        near = jnp.where(col < R, col, col + CZ)
        got = jnp.where(col < 2 * R, pick(taps, base, near - row), 0.0)
        high, low = split(got)
        tz1[v, :LANES, LANES:] = high
        tz1[v, LANES:, LANES:] = high
        tz2[v, :, LANES:] = low
        return carry

    lax.fori_loop(0, V, z_of, 0)


BANDS = ((0, 8), (8, 24), (24, 32))


def main_kernel(
    flag, taps, field, w9, z1, z2, observed, w_own, by, byt, wz1, wz2, tz1, tz2,
    part, op1, op2, sums,
    et, gs, hs, xs, ys, wy, edge, edges, ws,
):
    odd_z = flag[2] == 1
    one, two = z1[...], z2[...]
    below, above = jnp.where(odd_z, one, two), jnp.where(odd_z, two, one)
    for b in range(2):
        cols = slice(ROWS + b * LANES, ROWS + (b + 1) * LANES)
        ws[b * 8 : b * 8 + 8] = below[:, cols]
        ws[32 + b * 8 : 40 + b * 8] = above[:, cols]
    ws[16:32] = w9[...]

    edges[:R] = below[:, :ROWS]
    edges[R:] = above[:, :ROWS]
    e = edges[...]
    et[...] = jnp.transpose(
        jnp.concatenate([e, e, e, jnp.zeros((LANES - 6 * R, ROWS), F32)], axis=0)
    )

    for bx in range(3):
        for zb in range(3):
            for j in range(3):
                at = zb * 16 + j * 3 + bx
                w_row = ws[at : at + 1, :]
                for q in range(BANDS[j][0], BANDS[j][1], 8):
                    rows = slice(zb * EY + q, zb * EY + q + 8)
                    high = w_row * byt[q : q + 8]
                    low = w_row * byt[EY + q : EY + q + 8]
                    wy[bx, rows, :LANES] = high
                    wy[bx, rows, LANES : 2 * LANES] = high
                    wy[bx, rows, 2 * LANES :] = low

    face = iota((LANES, LANES), 1)
    face_low = (face >= 2 * R) & (face < 4 * R)
    lhs = by[:, : 3 * EY]
    for x in range(EX):
        high, low = split(field[x])
        e_high, e_low = split(et[x * EY : (x + 1) * EY, :])
        top = jnp.concatenate([high, e_high], axis=1)
        rhs = jnp.concatenate([top, jnp.concatenate([low, e_low], axis=1), top], axis=0)
        got = jnp.dot(lhs, rhs, preferred_element_type=F32)
        high, low = split(got[:, :LANES])
        gs[:, x, :, :LANES] = high.reshape(V, CY, LANES)
        gs[:, x, :, LANES : 2 * LANES] = low.reshape(V, CY, LANES)
        e_got = got[:, LANES:]
        e_high = e_got.astype(BF16).astype(F32)
        both = jnp.where(face_low, e_got - e_high, e_high).astype(BF16)
        gs[:, x, :, 2 * LANES :] = both.reshape(V, CY, LANES)

    lane = iota((8, LANES), 1)
    seen = jnp.zeros((8, LANES), F32)
    for v in range(V):
        block = gs[v].reshape(EX * CY, 3 * LANES)
        got = jnp.dot(block[:, : 2 * LANES], wz1[v], preferred_element_type=F32)
        second = jnp.concatenate([block[:, :LANES], block[:, 2 * LANES :]], axis=1)
        got += jnp.dot(second, wz2[v], preferred_element_type=F32)
        hs[v] = got.reshape(EX, CY, LANES)
    for v in range(V):
        t = [taps[v * 3 * K + k] for k in range(K)]
        own = w_own[v : v + 1, :]
        for b in range(0, CY, 8):
            rows = slice(b, b + 8)
            for a in range(CX):
                acc = t[0] * hs[v, a, rows]
                for k in range(1, K):
                    acc += t[k] * hs[v, a + k, rows]
                image = observed[v, a, rows]
                seen = seen + own * image
                xs[v, a, rows] = image / acc
        for i in range(EX):
            acc = None
            for a in range(max(0, i - K + 1), min(CX, i + 1)):
                term = t[i - a] * xs[v, a]
                acc = term if acc is None else acc + term
            high, low = split(acc)
            gs[v, i, :, :LANES] = high
            gs[v, i, :, LANES : 2 * LANES] = low
        block = gs[v].reshape(EX * CY, 3 * LANES)
        got = jnp.dot(block[:, : 2 * LANES], tz1[v], preferred_element_type=F32)
        got += jnp.dot(block[:, :LANES], tz2[v], preferred_element_type=F32)
        high, low = split(got)
        ys[:, v * CY : (v + 1) * CY, :] = high.reshape(EX, CY, 2 * LANES)
        ys[:, (V + v) * CY : (V + v + 1) * CY, :] = low.reshape(EX, CY, 2 * LANES)

    sub = iota((EY, LANES), 1)
    for x in range(EX):
        bx = 0 if x < R else (1 if x < R + CX else 2)
        got = jnp.dot(wy[bx, :, : 2 * LANES].astype(BF16), ys[x], preferred_element_type=F32)
        got += jnp.dot(
            wy[bx, :, 2 * LANES :].astype(BF16), ys[x, : V * CY], preferred_element_type=F32
        )
        part[x] = got[EY : 2 * EY, :LANES]
        edge[x * EY : (x + 1) * EY, :] = jnp.where(
            sub < R, got[:EY, LANES:], got[2 * EY :, LANES:]
        )

    turned = jnp.transpose(edge[...])
    low, high = turned[:R], turned[R : 2 * R]
    op1[...] = jnp.where(odd_z, low, high)
    op2[...] = jnp.where(odd_z, high, low)

    def count_of(zb, at):
        row = ws[zb * 16 + at : zb * 16 + at + 1, :]
        return jnp.maximum(jnp.sum(row, axis=1, keepdims=True) * (1.0 / CY), 1.0)

    total = jnp.zeros((8, LANES), F32)
    place = iota((8, ROWS), 1) % EY
    y_band = jnp.where(place < R, 0, jnp.where(place < R + CY, 1, 2))
    low_sum = edges[:R] * low
    high_sum = edges[R:] * high
    for bx in range(3):
        x0, x1 = BANDS[bx]
        for j in range(3):
            y0, y1 = BANDS[j]
            at = j * 3 + bx
            block = (field[x0:x1, y0:y1] * part[x0:x1, y0:y1]).reshape((-1, 8, LANES))
            total += jnp.sum(block, axis=0) / count_of(1, at)
            lanes = slice(x0 * EY, x1 * EY)
            picked = y_band[:, lanes] == j
            for side, zb in ((low_sum, 0), (high_sum, 2)):
                cut = jnp.where(picked, side[:, lanes], 0.0)
                folded = cut[:, :LANES]
                for q in range(1, cut.shape[1] // LANES):
                    folded = folded + cut[:, q * LANES : (q + 1) * LANES]
                total += folded / count_of(zb, at)
    target = seen / count_of(1, 4)
    both = jnp.where(lane < 64, total_of(target), total_of(total))
    for p in range(sums.shape[0]):
        sums[p] = both


def z_add(flag, part, r1, r2, mid, op1, op2):
    odd_y, odd_z = flag[1] == 1, flag[2] == 1
    one, two = r1[...], r2[...]
    below, above = jnp.where(odd_z, one, two), jnp.where(odd_z, two, one)
    stacked = jnp.concatenate([below, jnp.zeros((CZ - 2 * R, ROWS), F32), above], axis=0)
    added = jnp.transpose(stacked).reshape(EX, EY, LANES)
    for i in range(EX):
        plane = part[i] + added[i]
        mid[i] = plane[R : R + CY]
        low, high = plane[:R], plane[R + CY :]
        op1[i * R : (i + 1) * R, :] = jnp.where(odd_y, low, high)
        op2[i * R : (i + 1) * R, :] = jnp.where(odd_y, high, low)


def y_add(flag, part, r1, r2, mid, op1, op2):
    odd_x, odd_y = flag[0] == 1, flag[1] == 1
    for i in range(EX):
        one, two = r1[i * R : (i + 1) * R], r2[i * R : (i + 1) * R]
        first = part[i, :R] + jnp.where(odd_y, one, two)
        second = part[i, R:] + jnp.where(odd_y, two, one)
        if i < R:
            at = i
            rows = slice(at * CY, at * CY + R), slice(at * CY + R, (at + 1) * CY)
            op2[rows[0], :] = first
            op2[rows[1], :] = second
        elif i < R + CX:
            mid[i - R, :R] = first
            mid[i - R, R:] = second
        else:
            at = i - R - CX
            rows = slice(at * CY, at * CY + R), slice(at * CY + R, (at + 1) * CY)
            for row, new in zip(rows, (first, second)):
                low = op2[row, :]
                op1[row, :] = jnp.where(odd_x, low, new)
                op2[row, :] = jnp.where(odd_x, new, low)


def x_add(flag, part, r1, r2, est, count, sums, out):
    odd_x = flag[0] == 1
    gathered = jnp.sum(sums[...], axis=0)[:1]
    lane = lax.broadcasted_iota(jnp.int32, (1, LANES), 1)
    target = jnp.sum(jnp.where(lane == 0, gathered, 0.0), axis=1, keepdims=True)
    total = jnp.sum(jnp.where(lane == 64, gathered, 0.0), axis=1, keepdims=True)
    scale = target / total
    counts = jnp.sum(count[...], axis=0, keepdims=True)
    for a in range(CX):
        rows = slice((a % R) * CY, (a % R + 1) * CY)
        one, two = r1[rows, :], r2[rows, :]
        got = jnp.where(odd_x, one, two) if a < R else jnp.where(odd_x, two, one)
        out[a] = est[a] * ((part[a] + got) / counts) * scale


def on_device(estimate, observed, coverage, psf_taps):
    taps = (psf_taps / jnp.sum(psf_taps, axis=2, keepdims=True)).reshape(-1)
    flag = jnp.stack([lax.axis_index(axis) % 2 for axis in ALL]).astype(jnp.int32)
    cover = coverage.reshape(V).astype(F32)
    w_own = jnp.broadcast_to(cover[:, None], (V, LANES))
    w_row = jnp.broadcast_to(jnp.repeat(cover, CY)[None], (8, LANES))
    peers = lax.axis_size(ALL)

    op = shape(R * CY + 8, LANES)
    x1, x2 = kernel_call(x_pack, (op, op), n_in=3, in_smem=1)(flag, estimate, w_row)
    x1, x2 = swap(x1, x2, "bx")
    tables = kernel_call(
        bands,
        (
            shape(V * CY, LANES, dtype=BF16),
            shape(2 * EY, LANES),
            shape(V, 2 * LANES, LANES, dtype=BF16),
            shape(V, 2 * LANES, LANES, dtype=BF16),
            shape(V, 2 * LANES, 2 * LANES, dtype=BF16),
            shape(V, LANES, 2 * LANES, dtype=BF16),
        ),
        n_in=1,
        in_smem=1,
        flops=2 * 10**8,
    )(taps)
    op = shape(EX * R + 8, LANES)
    fx, wx, y1, y2 = kernel_call(
        y_pack, (shape(EX, CY, LANES), shape(8, LANES), op, op), n_in=5, in_smem=1
    )(flag, estimate, w_row, x1, x2)
    y1, y2 = swap(y1, y2, "by")
    op = shape(R, ROWS + 2 * LANES)
    field, w9, z1, z2 = kernel_call(
        z_pack, (shape(EX, EY, LANES), shape(16, LANES), op, op), n_in=5, in_smem=1
    )(flag, fx, wx, y1, y2)
    z1, z2 = swap(z1, z2, "bz")

    face = shape(R, ROWS)
    part, z1, z2, sums = kernel_call(
        main_kernel,
        (shape(EX, EY, LANES), face, face, shape(peers, 8, LANES)),
        scratch=(
            pltpu.VMEM((ROWS, LANES), F32),
            pltpu.VMEM((V, EX, CY, 3 * LANES), BF16),
            pltpu.VMEM((V, EX, CY, LANES), F32),
            pltpu.VMEM((V, CX, CY, LANES), F32),
            pltpu.VMEM((EX, 2 * V * CY, 2 * LANES), BF16),
            pltpu.VMEM((3, 3 * EY, 3 * LANES), F32),
            pltpu.VMEM((ROWS, LANES), F32),
            pltpu.VMEM((2 * R, ROWS), F32),
            pltpu.VMEM((48, LANES), F32),
        ),
        n_in=14,
        in_smem=2,
        flops=2 * 10**9,
    )(flag, taps, field, w9, z1, z2, observed, w_own, *tables)

    sums = lax.all_to_all(sums, ALL, 0, 0)
    z1, z2 = swap(z1, z2, "bz")
    op = shape(EX * R, LANES)
    part, y1, y2 = kernel_call(z_add, (shape(EX, CY, LANES), op, op), n_in=4, in_smem=1)(
        flag, part, z1, z2
    )
    y1, y2 = swap(y1, y2, "by")
    op = shape(R * CY, LANES)
    part, x1, x2 = kernel_call(y_add, (shape(CX, CY, LANES), op, op), n_in=4, in_smem=1)(
        flag, part, y1, y2
    )
    x1, x2 = swap(x1, x2, "bx")
    return kernel_call(x_add, shape(CX, CY, LANES), n_in=7, in_smem=1)(
        flag, part, x1, x2, estimate, w_own, sums
    )


def solution(mesh):
    spec = P("bx", "by", "bz")
    views_spec = P(None, "bx", "by", "bz")
    return jax.shard_map(
        on_device,
        mesh=mesh,
        in_specs=(spec, views_spec, views_spec, P()),
        out_specs=spec,
        check_vma=False,
    )
```

```python
import jax
import jax.numpy as jnp
from jax import lax
from jax.experimental import pallas as pl
from jax.experimental.pallas import tpu as pltpu
from jax.sharding import PartitionSpec as P


ALL = ("bx", "by", "bz")
F32, BF16 = jnp.float32, jnp.bfloat16
V, R, K = 8, 8, 17
CX, CY, CZ = 16, 16, 128
EX, EY = CX + 2 * R, CY + 2 * R
ROWS = EX * EY
LANES = 128


def pairs(count, first):
    both = []
    for i in range(first, count - 1, 2):
        both += [(i, i + 1), (i + 1, i)]
    return both


def swap(one, two, axis):
    count = lax.axis_size(axis)
    return lax.ppermute(one, axis, pairs(count, 0)), lax.ppermute(two, axis, pairs(count, 1))


def kernel_call(body, out_shape, scratch=(), in_smem=0, flops=0, n_in=0):
    vmem = pl.BlockSpec(memory_space=pltpu.VMEM)
    smem = pl.BlockSpec(memory_space=pltpu.SMEM)
    return pl.pallas_call(
        body,
        out_shape=out_shape,
        in_specs=[smem] * in_smem + [vmem] * (n_in - in_smem),
        out_specs=jax.tree.map(lambda _: vmem, out_shape),
        scratch_shapes=list(scratch),
        compiler_params=pltpu.CompilerParams(vmem_limit_bytes=48 * 1024 * 1024),
        cost_estimate=pl.CostEstimate(flops=flops, bytes_accessed=1024, transcendentals=0),
    )


def shape(*dims, dtype=F32):
    return jax.ShapeDtypeStruct(dims, dtype)


def spread_cover(cover):
    lane = iota((8, LANES), 1) // CY
    row = jnp.zeros((8, LANES), F32)
    for v in range(V):
        row = jnp.where(lane == v, cover[v].astype(F32), row)
    return row


def y_pack(flag, cover, est, op1, op2):
    odd = flag[1] == 1
    for i in range(CX):
        low, high = est[i, :R], est[i, CY - R :]
        op1[i * R : (i + 1) * R, :] = jnp.where(odd, low, high)
        op2[i * R : (i + 1) * R, :] = jnp.where(odd, high, low)
    row = spread_cover(cover)
    op1[CX * R :, :] = row
    op2[CX * R :, :] = row


def x_pack(flag, cover, est, y1, y2, field, ws, op1, op2):
    odd_x, odd_y = flag[0] == 1, flag[1] == 1
    one, two = y1[...], y2[...]
    below, above = jnp.where(odd_y, one, two), jnp.where(odd_y, two, one)
    cells = CX * R
    field[:, :R] = below[:cells].reshape(CX, R, LANES)
    field[:, R : R + CY] = est[...]
    field[:, R + CY :] = above[:cells].reshape(CX, R, LANES)
    ws[...] = jnp.zeros_like(ws)
    ws[:1] = below[cells : cells + 1]
    ws[1:2] = spread_cover(cover)[:1]
    ws[2:3] = above[cells : cells + 1]
    for a in range(R):
        low, high = field[a], field[CX - R + a]
        op1[a * EY : (a + 1) * EY, :] = jnp.where(odd_x, low, high)
        op2[a * EY : (a + 1) * EY, :] = jnp.where(odd_x, high, low)
    op1[R * EY :, :] = ws[...]
    op2[R * EY :, :] = ws[...]


def z_pack(flag, fy, wy, x1, x2, field, ws, op1, op2):
    odd_x, odd_z = flag[0] == 1, flag[2] == 1
    one, two = x1[...], x2[...]
    below, above = jnp.where(odd_x, one, two), jnp.where(odd_x, two, one)
    cells = R * EY
    field[:R] = below[:cells].reshape(R, EY, LANES)
    field[R : R + CX] = fy[...]
    field[R + CX :] = above[:cells].reshape(R, EY, LANES)
    ws[...] = jnp.zeros_like(ws)
    ws[:3] = below[cells : cells + 3]
    ws[3:6] = wy[:3]
    ws[6:9] = above[cells : cells + 3]
    turned = jnp.transpose(field[...].reshape(ROWS, LANES))
    low, high = turned[:R], turned[CZ - R :]
    op1[:, :ROWS] = jnp.where(odd_z, low, high)
    op2[:, :ROWS] = jnp.where(odd_z, high, low)
    for b in range(2):
        cols = slice(ROWS + b * LANES, ROWS + (b + 1) * LANES)
        op1[:, cols] = ws[b * 8 : b * 8 + 8]
        op2[:, cols] = ws[b * 8 : b * 8 + 8]


def total_of(x):
    return jnp.sum(jnp.sum(x, axis=0, keepdims=True), axis=1, keepdims=True)


def split(x):
    high = x.astype(BF16)
    return high, (x - high.astype(F32)).astype(BF16)


def iota(dims, axis):
    return lax.broadcasted_iota(jnp.int32, dims, axis)


def pick(taps, v, d, offset, scale):
    got = jnp.zeros(offset.shape, F32)
    for k in range(K):
        got = jnp.where(offset == k, taps[v, d, k], got)
    return got * scale


def inverse_sum(taps, v, d):
    total = taps[v, d, 0]
    for k in range(1, K):
        total = total + taps[v, d, k]
    return 1.0 / jnp.full((8, LANES), total, F32)[:1]


def bands(taps, by, byt, wz1, wz2, tz1, tz2):
    for v in range(V):
        rows = slice(v * CY, (v + 1) * CY)
        scale = inverse_sum(taps, v, 0) * inverse_sum(taps, v, 1)
        column = iota((CY, LANES), 1)
        got = pick(taps, v, 1, column % EY - iota((CY, LANES), 0), scale)
        high, low = split(got)
        by[rows, :] = jnp.where(column < 2 * EY, high.astype(F32), low.astype(F32)).astype(BF16)

    def turned_y(v, got):
        lane = iota((EY, LANES), 1)
        scale = inverse_sum(taps, v, 0) * inverse_sum(taps, v, 1)
        here = pick(taps, v, 1, iota((EY, LANES), 0) - lane % CY, scale)
        return jnp.where(lane // CY == v, here, got)

    both = lax.fori_loop(0, V, turned_y, jnp.zeros((EY, LANES), F32))
    high, low = split(both)
    byt[:EY, :] = high.astype(F32)
    byt[EY:, :] = low.astype(F32)

    def z_of(v, carry):
        scale = inverse_sum(taps, v, 2)
        row, col = iota((LANES, LANES), 0), iota((LANES, LANES), 1)
        high, low = split(pick(taps, v, 2, row + R - col, scale))
        wz1[v, :LANES, :] = high
        wz1[v, LANES:, :] = high
        wz2[v, :LANES, :] = low
        place = row[: 6 * R] % (2 * R)
        near = jnp.where(place < R, place, place + CZ)
        got = pick(taps, v, 2, near - col[: 6 * R], scale)
        high, low = split(got)
        which = row[: 6 * R] < 4 * R
        wz2[v, LANES : LANES + 6 * R, :] = jnp.where(
            which, high.astype(F32), low.astype(F32)
        ).astype(BF16)
        wz2[v, LANES + 6 * R :, :] = jnp.zeros((LANES - 6 * R, LANES), BF16)
        high, low = split(pick(taps, v, 2, col + R - row, scale))
        tz1[v, :LANES, :LANES] = high
        tz1[v, LANES:, :LANES] = high
        tz2[v, :, :LANES] = low
        near = jnp.where(col < R, col, col + CZ)
        got = jnp.where(col < 2 * R, pick(taps, v, 2, near - row, scale), 0.0)
        high, low = split(got)
        tz1[v, :LANES, LANES:] = high
        tz1[v, LANES:, LANES:] = high
        tz2[v, :, LANES:] = low
        return carry

    lax.fori_loop(0, V, z_of, 0)


BANDS = ((0, 8), (8, 24), (24, 32))


def main_kernel(
    flag, taps, cover, field, w9, z1, z2, observed, by, byt, wz1, wz2, tz1, tz2,
    part, op1, op2, sums,
    et, gs, hs, xs, ys, wy, edge, edges, ws,
):
    odd_z = flag[2] == 1
    one, two = z1[...], z2[...]
    below, above = jnp.where(odd_z, one, two), jnp.where(odd_z, two, one)
    for b in range(2):
        cols = slice(ROWS + b * LANES, ROWS + (b + 1) * LANES)
        ws[b * 8 : b * 8 + 8] = below[:, cols]
        ws[32 + b * 8 : 40 + b * 8] = above[:, cols]
    ws[16:32] = w9[...]

    edges[:R] = below[:, :ROWS]
    edges[R:] = above[:, :ROWS]
    e = edges[...]
    et[...] = jnp.transpose(
        jnp.concatenate([e, e, e, jnp.zeros((LANES - 6 * R, ROWS), F32)], axis=0)
    )

    for bx in range(3):
        for zb in range(3):
            for j in range(3):
                at = zb * 16 + bx * 3 + j
                w_row = ws[at : at + 1, :]
                for q in range(BANDS[j][0], BANDS[j][1], 8):
                    rows = slice(zb * EY + q, zb * EY + q + 8)
                    high = w_row * byt[q : q + 8]
                    low = w_row * byt[EY + q : EY + q + 8]
                    wy[bx, rows, :LANES] = high
                    wy[bx, rows, LANES : 2 * LANES] = high
                    wy[bx, rows, 2 * LANES :] = low

    face = iota((LANES, LANES), 1)
    face_low = (face >= 2 * R) & (face < 4 * R)
    lhs = by[:, : 3 * EY]
    for x in range(EX):
        high, low = split(field[x])
        e_high, e_low = split(et[x * EY : (x + 1) * EY, :])
        top = jnp.concatenate([high, e_high], axis=1)
        rhs = jnp.concatenate([top, jnp.concatenate([low, e_low], axis=1), top], axis=0)
        got = jnp.dot(lhs, rhs, preferred_element_type=F32)
        high, low = split(got[:, :LANES])
        gs[:, x, :, :LANES] = high.reshape(V, CY, LANES)
        gs[:, x, :, LANES : 2 * LANES] = low.reshape(V, CY, LANES)
        e_got = got[:, LANES:]
        e_high = e_got.astype(BF16).astype(F32)
        both = jnp.where(face_low, e_got - e_high, e_high).astype(BF16)
        gs[:, x, :, 2 * LANES :] = both.reshape(V, CY, LANES)

    lane = iota((8, LANES), 1)
    seen = jnp.zeros((8, LANES), F32)
    for v in range(V):
        block = gs[v].reshape(EX * CY, 3 * LANES)
        got = jnp.dot(block[:, : 2 * LANES], wz1[v], preferred_element_type=F32)
        second = jnp.concatenate([block[:, :LANES], block[:, 2 * LANES :]], axis=1)
        got += jnp.dot(second, wz2[v], preferred_element_type=F32)
        hs[v] = got.reshape(EX, CY, LANES)
    for v in range(V):
        t = [taps[v, 0, k] for k in range(K)]
        own = cover[v].astype(F32)
        for b in range(0, CY, 8):
            rows = slice(b, b + 8)
            for a in range(CX):
                acc = t[0] * hs[v, a, rows]
                for k in range(1, K):
                    acc += t[k] * hs[v, a + k, rows]
                image = observed[v, a, rows]
                seen = seen + own * image
                xs[v, a, rows] = image / acc
        for i in range(EX):
            acc = None
            for a in range(max(0, i - K + 1), min(CX, i + 1)):
                term = t[i - a] * xs[v, a]
                acc = term if acc is None else acc + term
            high, low = split(acc)
            gs[v, i, :, :LANES] = high
            gs[v, i, :, LANES : 2 * LANES] = low
        block = gs[v].reshape(EX * CY, 3 * LANES)
        got = jnp.dot(block[:, : 2 * LANES], tz1[v], preferred_element_type=F32)
        got += jnp.dot(block[:, :LANES], tz2[v], preferred_element_type=F32)
        high, low = split(got)
        ys[:, v * CY : (v + 1) * CY, :] = high.reshape(EX, CY, 2 * LANES)
        ys[:, (V + v) * CY : (V + v + 1) * CY, :] = low.reshape(EX, CY, 2 * LANES)

    sub = iota((EY, LANES), 1)
    for x in range(EX):
        bx = 0 if x < R else (1 if x < R + CX else 2)
        got = jnp.dot(wy[bx, :, : 2 * LANES].astype(BF16), ys[x], preferred_element_type=F32)
        got += jnp.dot(
            wy[bx, :, 2 * LANES :].astype(BF16), ys[x, : V * CY], preferred_element_type=F32
        )
        part[x] = got[EY : 2 * EY, :LANES]
        edge[x * EY : (x + 1) * EY, :] = jnp.where(
            sub < R, got[:EY, LANES:], got[2 * EY :, LANES:]
        )

    turned = jnp.transpose(edge[...])
    low, high = turned[:R], turned[R : 2 * R]
    op1[...] = jnp.where(odd_z, low, high)
    op2[...] = jnp.where(odd_z, high, low)

    def count_of(zb, at):
        row = ws[zb * 16 + at : zb * 16 + at + 1, :]
        return jnp.maximum(jnp.sum(row, axis=1, keepdims=True) * (1.0 / CY), 1.0)

    total = jnp.zeros((8, LANES), F32)
    place = iota((8, ROWS), 1) % EY
    y_band = jnp.where(place < R, 0, jnp.where(place < R + CY, 1, 2))
    low_sum = edges[:R] * low
    high_sum = edges[R:] * high
    for bx in range(3):
        x0, x1 = BANDS[bx]
        for j in range(3):
            y0, y1 = BANDS[j]
            at = bx * 3 + j
            block = (field[x0:x1, y0:y1] * part[x0:x1, y0:y1]).reshape((-1, 8, LANES))
            total += jnp.sum(block, axis=0) / count_of(1, at)
            lanes = slice(x0 * EY, x1 * EY)
            picked = y_band[:, lanes] == j
            for side, zb in ((low_sum, 0), (high_sum, 2)):
                cut = jnp.where(picked, side[:, lanes], 0.0)
                folded = cut[:, :LANES]
                for q in range(1, cut.shape[1] // LANES):
                    folded = folded + cut[:, q * LANES : (q + 1) * LANES]
                total += folded / count_of(zb, at)
    target = seen / count_of(1, 4)
    both = jnp.where(lane < 64, total_of(target), total_of(total))
    for p in range(sums.shape[0]):
        sums[p] = both


def z_add(flag, part, r1, r2, mid, op1, op2):
    odd_x, odd_z = flag[0] == 1, flag[2] == 1
    one, two = r1[...], r2[...]
    below, above = jnp.where(odd_z, one, two), jnp.where(odd_z, two, one)
    stacked = jnp.concatenate([below, jnp.zeros((CZ - 2 * R, ROWS), F32), above], axis=0)
    added = jnp.transpose(stacked).reshape(EX, EY, LANES)
    mid[...] = part[R : R + CX] + added[R : R + CX]
    for i in range(R):
        low, high = part[i] + added[i], part[R + CX + i] + added[R + CX + i]
        op1[i * EY : (i + 1) * EY, :] = jnp.where(odd_x, low, high)
        op2[i * EY : (i + 1) * EY, :] = jnp.where(odd_x, high, low)


def x_add(flag, part, r1, r2, mid, op1, op2):
    odd_x, odd_y = flag[0] == 1, flag[1] == 1
    for a in range(CX):
        rows = slice((a % R) * EY, (a % R + 1) * EY)
        one, two = r1[rows, :], r2[rows, :]
        plane = part[a] + (jnp.where(odd_x, one, two) if a < R else jnp.where(odd_x, two, one))
        mid[a] = plane[R : R + CY]
        low, high = plane[:R], plane[R + CY :]
        op1[a * R : (a + 1) * R, :] = jnp.where(odd_y, low, high)
        op2[a * R : (a + 1) * R, :] = jnp.where(odd_y, high, low)


def scale_of(cover, sums, scale):
    gathered = jnp.sum(sums[...], axis=0)
    lane = iota((8, LANES), 1)
    target = jnp.sum(jnp.where(lane == 0, gathered, 0.0), axis=1, keepdims=True)
    total = jnp.sum(jnp.where(lane == 64, gathered, 0.0), axis=1, keepdims=True)
    count = jnp.sum(spread_cover(cover), axis=1, keepdims=True) * (1.0 / CY)
    scale[...] = jnp.broadcast_to(target / total / count, (8, LANES))


def y_add(flag, part, r1, r2, est, scale, out):
    odd = flag[1] == 1
    by = scale[...]
    for a in range(CX):
        one, two = r1[a * R : (a + 1) * R, :], r2[a * R : (a + 1) * R, :]
        out[a, :R] = est[a, :R] * (part[a, :R] + jnp.where(odd, one, two)) * by
        out[a, R:] = est[a, R:] * (part[a, R:] + jnp.where(odd, two, one)) * by


def on_device(estimate, observed, coverage, psf_taps):
    flag = jnp.stack([lax.axis_index(axis) % 2 for axis in ALL]).astype(jnp.int32)
    cover = coverage.reshape(V)
    peers = lax.axis_size(ALL)

    op = shape(R * CX + 8, LANES)
    y1, y2 = kernel_call(y_pack, (op, op), n_in=3, in_smem=2)(flag, cover, estimate)
    y1, y2 = swap(y1, y2, "by")
    tables = kernel_call(
        bands,
        (
            shape(V * CY, LANES, dtype=BF16),
            shape(2 * EY, LANES),
            shape(V, 2 * LANES, LANES, dtype=BF16),
            shape(V, 2 * LANES, LANES, dtype=BF16),
            shape(V, 2 * LANES, 2 * LANES, dtype=BF16),
            shape(V, LANES, 2 * LANES, dtype=BF16),
        ),
        n_in=1,
        in_smem=1,
        flops=2 * 10**8,
    )(psf_taps)
    op = shape(EY * R + 8, LANES)
    fy, wy, x1, x2 = kernel_call(
        x_pack, (shape(CX, EY, LANES), shape(8, LANES), op, op), n_in=5, in_smem=2
    )(flag, cover, estimate, y1, y2)
    x1, x2 = swap(x1, x2, "bx")
    op = shape(R, ROWS + 2 * LANES)
    field, w9, z1, z2 = kernel_call(
        z_pack, (shape(EX, EY, LANES), shape(16, LANES), op, op), n_in=5, in_smem=1
    )(flag, fy, wy, x1, x2)
    z1, z2 = swap(z1, z2, "bz")

    face = shape(R, ROWS)
    part, z1, z2, sums = kernel_call(
        main_kernel,
        (shape(EX, EY, LANES), face, face, shape(peers, 8, LANES)),
        scratch=(
            pltpu.VMEM((ROWS, LANES), F32),
            pltpu.VMEM((V, EX, CY, 3 * LANES), BF16),
            pltpu.VMEM((V, EX, CY, LANES), F32),
            pltpu.VMEM((V, CX, CY, LANES), F32),
            pltpu.VMEM((EX, 2 * V * CY, 2 * LANES), BF16),
            pltpu.VMEM((3, 3 * EY, 3 * LANES), F32),
            pltpu.VMEM((ROWS, LANES), F32),
            pltpu.VMEM((2 * R, ROWS), F32),
            pltpu.VMEM((48, LANES), F32),
        ),
        n_in=14,
        in_smem=3,
        flops=2 * 10**9,
    )(flag, psf_taps, cover, field, w9, z1, z2, observed, *tables)

    z1, z2 = swap(z1, z2, "bz")
    sums = lax.all_to_all(sums, ALL, 0, 0)
    op = shape(EY * R, LANES)
    part, x1, x2 = kernel_call(z_add, (shape(CX, EY, LANES), op, op), n_in=4, in_smem=1)(
        flag, part, z1, z2
    )
    x1, x2 = swap(x1, x2, "bx")
    scale = kernel_call(scale_of, shape(8, LANES), n_in=2, in_smem=1, flops=10**6)(cover, sums)
    op = shape(R * CX, LANES)
    part, y1, y2 = kernel_call(x_add, (shape(CX, CY, LANES), op, op), n_in=4, in_smem=1)(
        flag, part, x1, x2
    )
    y1, y2 = swap(y1, y2, "by")
    return kernel_call(y_add, shape(CX, CY, LANES), n_in=6, in_smem=1)(
        flag, part, y1, y2, estimate, scale
    )


def solution(mesh):
    spec = P("bx", "by", "bz")
    views_spec = P(None, "bx", "by", "bz")

    return jax.shard_map(
        on_device,
        mesh=mesh,
        in_specs=(spec, views_spec, views_spec, P()),
        out_specs=spec,
        check_vma=False,
    )
```

```python
import jax
import jax.numpy as jnp
from jax import lax
from jax.experimental import pallas as pl
from jax.experimental.pallas import tpu as pltpu
from jax.sharding import PartitionSpec as P


ALL = ("bx", "by", "bz")
F32, BF16 = jnp.float32, jnp.bfloat16
V, R, K = 8, 8, 17
CX, CY, CZ = 16, 16, 128
EX, EY = CX + 2 * R, CY + 2 * R
ROWS = EX * EY
LANES = 128


def pairs(count, first):
    both = []
    for i in range(first, count - 1, 2):
        both += [(i, i + 1), (i + 1, i)]
    return both


def swap(one, two, axis):
    count = lax.axis_size(axis)
    return lax.ppermute(one, axis, pairs(count, 0)), lax.ppermute(two, axis, pairs(count, 1))


def kernel_call(body, out_shape, scratch=(), in_smem=0, flops=0, n_in=0):
    vmem = pl.BlockSpec(memory_space=pltpu.VMEM)
    smem = pl.BlockSpec(memory_space=pltpu.SMEM)
    return pl.pallas_call(
        body,
        out_shape=out_shape,
        in_specs=[smem] * in_smem + [vmem] * (n_in - in_smem),
        out_specs=jax.tree.map(lambda _: vmem, out_shape),
        scratch_shapes=list(scratch),
        compiler_params=pltpu.CompilerParams(vmem_limit_bytes=48 * 1024 * 1024),
        cost_estimate=pl.CostEstimate(flops=flops, bytes_accessed=1024, transcendentals=0),
    )


def shape(*dims, dtype=F32):
    return jax.ShapeDtypeStruct(dims, dtype)


def spread_cover(cover):
    lane = iota((8, LANES), 1) // CY
    row = jnp.zeros((8, LANES), F32)
    for v in range(V):
        row = jnp.where(lane == v, cover[v].astype(F32), row)
    return row


def y_pack(flag, cover, est, op1, op2):
    odd = flag[1] == 1
    for i in range(CX):
        low, high = est[i, :R], est[i, CY - R :]
        op1[i * R : (i + 1) * R, :] = jnp.where(odd, low, high)
        op2[i * R : (i + 1) * R, :] = jnp.where(odd, high, low)
    row = spread_cover(cover)
    op1[CX * R :, :] = row
    op2[CX * R :, :] = row


def x_pack(flag, cover, est, y1, y2, field, ws, op1, op2):
    odd_x, odd_y = flag[0] == 1, flag[1] == 1
    one, two = y1[...], y2[...]
    below, above = jnp.where(odd_y, one, two), jnp.where(odd_y, two, one)
    cells = CX * R
    field[:, :R] = below[:cells].reshape(CX, R, LANES)
    field[:, R : R + CY] = est[...]
    field[:, R + CY :] = above[:cells].reshape(CX, R, LANES)
    ws[...] = jnp.zeros_like(ws)
    ws[:1] = below[cells : cells + 1]
    ws[1:2] = spread_cover(cover)[:1]
    ws[2:3] = above[cells : cells + 1]
    for a in range(R):
        low, high = field[a], field[CX - R + a]
        op1[a * EY : (a + 1) * EY, :] = jnp.where(odd_x, low, high)
        op2[a * EY : (a + 1) * EY, :] = jnp.where(odd_x, high, low)
    op1[R * EY :, :] = ws[...]
    op2[R * EY :, :] = ws[...]


def z_pack(flag, fy, wy, x1, x2, field, ws, op1, op2):
    odd_x, odd_z = flag[0] == 1, flag[2] == 1
    one, two = x1[...], x2[...]
    below, above = jnp.where(odd_x, one, two), jnp.where(odd_x, two, one)
    cells = R * EY
    field[:R] = below[:cells].reshape(R, EY, LANES)
    field[R : R + CX] = fy[...]
    field[R + CX :] = above[:cells].reshape(R, EY, LANES)
    ws[...] = jnp.zeros_like(ws)
    ws[:3] = below[cells : cells + 3]
    ws[3:6] = wy[:3]
    ws[6:9] = above[cells : cells + 3]
    turned = jnp.transpose(field[...].reshape(ROWS, LANES))
    low, high = turned[: 2 * R], turned[CZ - 2 * R :]
    op1[...] = jnp.where(odd_z, low, high)
    op2[...] = jnp.where(odd_z, high, low)


def image_pack(flag, observed, op1, op2):
    odd = flag[2] == 1
    for v in range(V):
        turned = jnp.transpose(observed[v].reshape(CX * CY, LANES))
        low, high = turned[:R], turned[CZ - R :]
        op1[v * R : (v + 1) * R, :] = jnp.where(odd, low, high)
        op2[v * R : (v + 1) * R, :] = jnp.where(odd, high, low)


def total_of(x):
    return jnp.sum(jnp.sum(x, axis=0, keepdims=True), axis=1, keepdims=True)


def split(x):
    high = x.astype(BF16)
    return high, (x - high.astype(F32)).astype(BF16)


def iota(dims, axis):
    return lax.broadcasted_iota(jnp.int32, dims, axis)


def pick(taps, v, d, offset, scale):
    got = jnp.zeros(offset.shape, F32)
    for k in range(K):
        got = jnp.where(offset == k, taps[v, d, k], got)
    return got * scale


def inverse_sum(taps, v, d):
    total = taps[v, d, 0]
    for k in range(1, K):
        total = total + taps[v, d, k]
    return 1.0 / jnp.full((8, LANES), total, F32)[:1]


def bands(taps, by, byt, wz1, wz2, tz1, tz2, tz3, tx):
    for v in range(V):
        rows = slice(v * CY, (v + 1) * CY)
        scale = inverse_sum(taps, v, 0) * inverse_sum(taps, v, 1)
        column = iota((CY, LANES), 1)
        got = pick(taps, v, 1, column % EY - iota((CY, LANES), 0), scale)
        high, low = split(got)
        by[rows, :] = jnp.where(column < 2 * EY, high.astype(F32), low.astype(F32)).astype(BF16)

    def turned_y(v, got):
        lane = iota((EY, LANES), 1)
        scale = inverse_sum(taps, v, 0) * inverse_sum(taps, v, 1)
        here = pick(taps, v, 1, iota((EY, LANES), 0) - lane % CY, scale)
        return jnp.where(lane // CY == v, here, got)

    both = lax.fori_loop(0, V, turned_y, jnp.zeros((EY, LANES), F32))
    high, low = split(both)
    byt[:EY, :] = high.astype(F32)
    byt[EY:, :] = low.astype(F32)

    owner = iota((8, LANES), 1) // (2 * R)
    for k in range(K):
        row = jnp.zeros((8, LANES), F32)
        for v in range(V):
            row = jnp.where(owner == v, taps[v, 0, k], row)
        tx[k : k + 1, :] = row[:1]
    tx[K:, :] = jnp.zeros((24 - K, LANES), F32)

    def z_of(v, carry):
        scale = inverse_sum(taps, v, 2)
        row, col = iota((LANES, LANES), 0), iota((LANES, LANES), 1)

        def slot(lane):
            place = lane - 2 * R * v
            z = jnp.where(place < R, place - R, place - R + CZ)
            return jnp.where((place >= 0) & (place < 2 * R), z, 4 * CZ)

        def past(lane):
            return jnp.where(lane < 2 * R, lane - 2 * R, lane - 2 * R + CZ)

        ends = row[: 12 * R]
        z_end = past(ends % (4 * R))
        first = ends < 8 * R
        for half, z_out in ((slice(0, LANES), col), (slice(LANES, 2 * LANES), slot(col))):
            high, low = split(pick(taps, v, 2, row - z_out + R, scale))
            wz1[v, :LANES, half] = high
            wz1[v, LANES:, half] = high
            wz2[v, :LANES, half] = low
            high, low = split(pick(taps, v, 2, z_end - z_out[: 12 * R] + R, scale))
            wz2[v, LANES : LANES + 12 * R, half] = jnp.where(
                first, high.astype(F32), low.astype(F32)
            ).astype(BF16)
            wz2[v, LANES + 12 * R :, half] = jnp.zeros((LANES - 12 * R, LANES), BF16)
        high, low = split(pick(taps, v, 2, col - row + R, scale))
        tz1[v, :LANES, :] = high
        tz1[v, LANES:, :] = high
        tz2[v, :LANES, :] = low
        high, low = split(pick(taps, v, 2, col - slot(row) + R, scale))
        tz2[v, LANES:, :] = high
        tz3[v, :LANES, :] = low
        tz3[v, LANES:, :] = high
        return carry

    lax.fori_loop(0, V, z_of, 0)


BANDS = ((0, 8), (8, 24), (24, 32))


def main_kernel(
    flag, taps, cover, field, w9, z1, z2, i1, i2, observed, by, byt, wz1, wz2, tz1, tz2, tz3, tx,
    mid, op1, op2, sums,
    et, image_e, gs, hs, hp, xs, xe, pe, ys, wy, part,
):
    odd_x, odd_z = flag[0] == 1, flag[2] == 1
    one, two = z1[...], z2[...]
    below, above = jnp.where(odd_z, one, two), jnp.where(odd_z, two, one)
    e = jnp.concatenate([below, above], axis=0)
    et[...] = jnp.transpose(
        jnp.concatenate([e, e, e, jnp.zeros((LANES - 12 * R, ROWS), F32)], axis=0)
    )
    one, two = i1[...], i2[...]
    below, above = jnp.where(odd_z, one, two), jnp.where(odd_z, two, one)
    rows_e = []
    for v in range(V):
        rows_e += [below[v * R : (v + 1) * R], above[v * R : (v + 1) * R]]
    image_e[...] = jnp.transpose(jnp.concatenate(rows_e, axis=0)).reshape(CX, CY, LANES)

    for bx in range(3):
        for j in range(3):
            w_row = w9[bx * 3 + j : bx * 3 + j + 1, :]
            for q in range(BANDS[j][0], BANDS[j][1], 8):
                rows = slice(q, q + 8)
                high = w_row * byt[q : q + 8]
                wy[bx, rows, :LANES] = high
                wy[bx, rows, LANES : 2 * LANES] = high
                wy[bx, rows, 2 * LANES :] = w_row * byt[EY + q : EY + q + 8]

    face = iota((LANES, LANES), 1)
    face_low = (face >= 4 * R) & (face < 8 * R)
    lhs = by[:, : 3 * EY]
    for x in range(EX):
        high, low = split(field[x])
        e_high, e_low = split(et[x * EY : (x + 1) * EY, :])
        top = jnp.concatenate([high, e_high], axis=1)
        rhs = jnp.concatenate([top, jnp.concatenate([low, e_low], axis=1), top], axis=0)
        got = jnp.dot(lhs, rhs, preferred_element_type=F32)
        high, low = split(got[:, :LANES])
        gs[:, x, :, :LANES] = high.reshape(V, CY, LANES)
        gs[:, x, :, LANES : 2 * LANES] = low.reshape(V, CY, LANES)
        e_got = got[:, LANES:]
        e_high = e_got.astype(BF16).astype(F32)
        both = jnp.where(face_low, e_got - e_high, e_high).astype(BF16)
        gs[:, x, :, 2 * LANES :] = both.reshape(V, CY, LANES)

    for v in range(V):
        block = gs[v].reshape(EX * CY, 3 * LANES)
        got = jnp.dot(block[:, : 2 * LANES], wz1[v], preferred_element_type=F32)
        second = jnp.concatenate([block[:, :LANES], block[:, 2 * LANES :]], axis=1)
        got += jnp.dot(second, wz2[v], preferred_element_type=F32)
        hs[v] = got[:, :LANES].reshape(EX, CY, LANES)
        ends = got[:, LANES:].reshape(EX, CY, LANES)
        if v == 0:
            hp[...] = ends
        else:
            hp[...] += ends

    for b in range(0, CY, 8):
        rows = slice(b, b + 8)
        for a in range(CX):
            acc = tx[0:1, :] * hp[a, rows]
            for k in range(1, K):
                acc += tx[k : k + 1, :] * hp[a + k, rows]
            xe[a, rows] = image_e[a, rows] / acc
    for i in range(EX):
        acc = None
        for a in range(max(0, i - K + 1), min(CX, i + 1)):
            term = tx[i - a : i - a + 1, :] * xe[a]
            acc = term if acc is None else acc + term
        high, low = split(acc)
        pe[i, :, :LANES] = high
        pe[i, :, LANES:] = low

    lane = iota((8, LANES), 1)
    seen = jnp.zeros((8, LANES), F32)
    packed = pe[...].reshape(EX * CY, 2 * LANES)
    for v in range(V):
        t = [taps[v, 0, k] for k in range(K)]
        own = cover[v].astype(F32)
        for b in range(0, CY, 8):
            rows = slice(b, b + 8)
            for a in range(CX):
                acc = t[0] * hs[v, a, rows]
                for k in range(1, K):
                    acc += t[k] * hs[v, a + k, rows]
                image = observed[v, a, rows]
                seen = seen + own * image
                xs[v, a, rows] = image / acc
        for i in range(EX):
            acc = None
            for a in range(max(0, i - K + 1), min(CX, i + 1)):
                term = t[i - a] * xs[v, a]
                acc = term if acc is None else acc + term
            high, low = split(acc)
            gs[v, i, :, :LANES] = high
            gs[v, i, :, LANES : 2 * LANES] = low
        block = gs[v].reshape(EX * CY, 3 * LANES)
        got = jnp.dot(block[:, : 2 * LANES], tz1[v], preferred_element_type=F32)
        second = jnp.concatenate([block[:, :LANES], packed[:, :LANES]], axis=1)
        got += jnp.dot(second, tz2[v], preferred_element_type=F32)
        got += jnp.dot(packed, tz3[v], preferred_element_type=F32)
        for q, piece in enumerate(split(got)):
            piece = piece.reshape(EX // 2, 2, CY, LANES)
            rows = slice((q * V + v) * CY, (q * V + v + 1) * CY)
            ys[:, rows, :LANES] = piece[:, 0]
            ys[:, rows, LANES:] = piece[:, 1]

    for x in range(0, EX, 2):
        bx = 0 if x < R else (1 if x < R + CX else 2)
        got = jnp.dot(
            wy[bx, :, : 2 * LANES].astype(BF16), ys[x // 2], preferred_element_type=F32
        )
        got += jnp.dot(
            wy[bx, :, 2 * LANES :].astype(BF16), ys[x // 2, : V * CY], preferred_element_type=F32
        )
        part[x] = got[:, :LANES]
        part[x + 1] = got[:, LANES:]

    mid[...] = part[R : R + CX]
    for i in range(R):
        low, high = part[i], part[R + CX + i]
        op1[i * EY : (i + 1) * EY, :] = jnp.where(odd_x, low, high)
        op2[i * EY : (i + 1) * EY, :] = jnp.where(odd_x, high, low)

    def count_of(at):
        row = w9[at : at + 1, :]
        return jnp.maximum(jnp.sum(row, axis=1, keepdims=True) * (1.0 / CY), 1.0)

    total = jnp.zeros((8, LANES), F32)
    for bx in range(3):
        x0, x1 = BANDS[bx]
        for j in range(3):
            y0, y1 = BANDS[j]
            block = (field[x0:x1, y0:y1] * part[x0:x1, y0:y1]).reshape((-1, 8, LANES))
            total += jnp.sum(block, axis=0) / count_of(bx * 3 + j)
    target = seen / count_of(4)
    both = jnp.where(lane < 64, total_of(target), total_of(total))[:4]
    for p in range(sums.shape[0]):
        sums[p] = both


def x_add(flag, part, r1, r2, mid, op1, op2):
    odd_x, odd_y = flag[0] == 1, flag[1] == 1
    for a in range(CX):
        rows = slice((a % R) * EY, (a % R + 1) * EY)
        one, two = r1[rows, :], r2[rows, :]
        plane = part[a] + (jnp.where(odd_x, one, two) if a < R else jnp.where(odd_x, two, one))
        mid[a] = plane[R : R + CY]
        low, high = plane[:R], plane[R + CY :]
        op1[a * R : (a + 1) * R, :] = jnp.where(odd_y, low, high)
        op2[a * R : (a + 1) * R, :] = jnp.where(odd_y, high, low)


def scale_of(cover, sums, scale):
    gathered = jnp.sum(sums[...], axis=0)[:1]
    lane = iota((1, LANES), 1)
    target = jnp.sum(jnp.where(lane == 0, gathered, 0.0), axis=1, keepdims=True)
    total = jnp.sum(jnp.where(lane == 64, gathered, 0.0), axis=1, keepdims=True)
    count = jnp.sum(spread_cover(cover)[:1], axis=1, keepdims=True) * (1.0 / CY)
    scale[...] = jnp.broadcast_to(target / total / count, (8, LANES))


def y_add(flag, part, r1, r2, est, scale, out):
    odd = flag[1] == 1
    by = scale[...]
    for a in range(CX):
        one, two = r1[a * R : (a + 1) * R, :], r2[a * R : (a + 1) * R, :]
        out[a, :R] = est[a, :R] * (part[a, :R] + jnp.where(odd, one, two)) * by
        out[a, R:] = est[a, R:] * (part[a, R:] + jnp.where(odd, two, one)) * by


def on_device(estimate, observed, coverage, psf_taps):
    flag = jnp.stack([lax.axis_index(axis) % 2 for axis in ALL]).astype(jnp.int32)
    cover = coverage.reshape(V)
    peers = lax.axis_size(ALL)

    op = shape(R * CX + 8, LANES)
    y1, y2 = kernel_call(y_pack, (op, op), n_in=3, in_smem=2)(flag, cover, estimate)
    y1, y2 = swap(y1, y2, "by")
    op = shape(V * R, CX * CY)
    i1, i2 = kernel_call(image_pack, (op, op), n_in=2, in_smem=1, flops=10**7)(flag, observed)
    i1, i2 = swap(i1, i2, "bz")
    square = shape(V, 2 * LANES, LANES, dtype=BF16)
    wide = shape(V, 2 * LANES, 2 * LANES, dtype=BF16)
    tables = kernel_call(
        bands,
        (
            shape(V * CY, LANES, dtype=BF16),
            shape(2 * EY, LANES),
            wide,
            wide,
            square,
            square,
            square,
            shape(24, LANES),
        ),
        n_in=1,
        in_smem=1,
        flops=2 * 10**8,
    )(psf_taps)
    op = shape(EY * R + 8, LANES)
    fy, wy, x1, x2 = kernel_call(
        x_pack, (shape(CX, EY, LANES), shape(8, LANES), op, op), n_in=5, in_smem=2
    )(flag, cover, estimate, y1, y2)
    x1, x2 = swap(x1, x2, "bx")
    op = shape(2 * R, ROWS)
    field, w9, z1, z2 = kernel_call(
        z_pack, (shape(EX, EY, LANES), shape(16, LANES), op, op), n_in=5, in_smem=1
    )(flag, fy, wy, x1, x2)
    z1, z2 = swap(z1, z2, "bz")

    op = shape(EY * R, LANES)
    part, x1, x2, sums = kernel_call(
        main_kernel,
        (shape(CX, EY, LANES), op, op, shape(peers, 4, LANES)),
        scratch=(
            pltpu.VMEM((ROWS, LANES), F32),
            pltpu.VMEM((CX, CY, LANES), F32),
            pltpu.VMEM((V, EX, CY, 3 * LANES), BF16),
            pltpu.VMEM((V, EX, CY, LANES), F32),
            pltpu.VMEM((EX, CY, LANES), F32),
            pltpu.VMEM((V, CX, CY, LANES), F32),
            pltpu.VMEM((CX, CY, LANES), F32),
            pltpu.VMEM((EX, CY, 2 * LANES), BF16),
            pltpu.VMEM((EX // 2, 2 * V * CY, 2 * LANES), BF16),
            pltpu.VMEM((3, EY, 3 * LANES), F32),
            pltpu.VMEM((EX, EY, LANES), F32),
        ),
        n_in=18,
        in_smem=3,
        flops=2 * 10**9,
    )(flag, psf_taps, cover, field, w9, z1, z2, i1, i2, observed, *tables)

    x1, x2 = swap(x1, x2, "bx")
    sums = lax.all_to_all(sums, ALL, 0, 0)
    scale = kernel_call(scale_of, shape(8, LANES), n_in=2, in_smem=1, flops=10**6)(cover, sums)
    op = shape(R * CX, LANES)
    part, y1, y2 = kernel_call(x_add, (shape(CX, CY, LANES), op, op), n_in=4, in_smem=1)(
        flag, part, x1, x2
    )
    y1, y2 = swap(y1, y2, "by")
    return kernel_call(y_add, shape(CX, CY, LANES), n_in=6, in_smem=1)(
        flag, part, y1, y2, estimate, scale
    )


def solution(mesh):
    spec = P("bx", "by", "bz")
    views_spec = P(None, "bx", "by", "bz")

    return jax.shard_map(
        on_device,
        mesh=mesh,
        in_specs=(spec, views_spec, views_spec, P()),
        out_specs=spec,
        check_vma=False,
    )
```

```python
import jax
import jax.numpy as jnp
from jax import lax
from jax.experimental import pallas as pl
from jax.experimental.pallas import tpu as pltpu
from jax.sharding import PartitionSpec as P


ALL = ("bx", "by", "bz")
F32, BF16 = jnp.float32, jnp.bfloat16
V, R, K = 8, 8, 17
CX, CY, CZ = 16, 16, 128
EX, EY = CX + 2 * R, CY + 2 * R
ROWS = EX * EY
LANES = 128


def pairs(count, first):
    both = []
    for i in range(first, count - 1, 2):
        both += [(i, i + 1), (i + 1, i)]
    return both


def swap(one, two, axis):
    count = lax.axis_size(axis)
    return lax.ppermute(one, axis, pairs(count, 0)), lax.ppermute(two, axis, pairs(count, 1))


def kernel_call(body, out_shape, scratch=(), in_smem=0, flops=0, n_in=0, in_hbm=0, mib=8):
    vmem = pl.BlockSpec(memory_space=pltpu.VMEM)
    smem = pl.BlockSpec(memory_space=pltpu.SMEM)
    hbm = pl.BlockSpec(memory_space=pltpu.HBM)
    return pl.pallas_call(
        body,
        out_shape=out_shape,
        in_specs=[smem] * in_smem + [hbm] * in_hbm + [vmem] * (n_in - in_smem - in_hbm),
        out_specs=jax.tree.map(lambda _: vmem, out_shape),
        scratch_shapes=list(scratch),
        compiler_params=pltpu.CompilerParams(vmem_limit_bytes=mib * 1024 * 1024),
        cost_estimate=pl.CostEstimate(flops=flops, bytes_accessed=1024, transcendentals=0),
    )


def shape(*dims, dtype=F32):
    return jax.ShapeDtypeStruct(dims, dtype)


def spread_cover(cover):
    lane = iota((8, LANES), 1) // CY
    row = jnp.zeros((8, LANES), F32)
    for v in range(V):
        row = jnp.where(lane == v, cover[v].astype(F32), row)
    return row


def y_pack(flag, cover_hbm, est_hbm, op1, op2, cover, est, sems):
    copies = (
        pltpu.make_async_copy(est_hbm, est, sems.at[0]),
        pltpu.make_async_copy(cover_hbm, cover, sems.at[1]),
    )
    for copy in copies:
        copy.start()
    for copy in copies:
        copy.wait()
    odd = flag[1] == 1
    for i in range(CX):
        low, high = est[i, :R], est[i, CY - R :]
        op1[i * R : (i + 1) * R, :] = jnp.where(odd, low, high)
        op2[i * R : (i + 1) * R, :] = jnp.where(odd, high, low)
    row = spread_cover(cover)
    op1[CX * R :, :] = row
    op2[CX * R :, :] = row


def x_pack(flag, cover, est, y1, y2, field, ws, op1, op2):
    odd_x, odd_y = flag[0] == 1, flag[1] == 1
    one, two = y1[...], y2[...]
    below, above = jnp.where(odd_y, one, two), jnp.where(odd_y, two, one)
    cells = CX * R
    field[:, :R] = below[:cells].reshape(CX, R, LANES)
    field[:, R : R + CY] = est[...]
    field[:, R + CY :] = above[:cells].reshape(CX, R, LANES)
    ws[...] = jnp.zeros_like(ws)
    ws[:1] = below[cells : cells + 1]
    ws[1:2] = spread_cover(cover)[:1]
    ws[2:3] = above[cells : cells + 1]
    for a in range(R):
        low, high = field[a], field[CX - R + a]
        op1[a * EY : (a + 1) * EY, :] = jnp.where(odd_x, low, high)
        op2[a * EY : (a + 1) * EY, :] = jnp.where(odd_x, high, low)
    op1[R * EY :, :] = ws[...]
    op2[R * EY :, :] = ws[...]


def z_pack(flag, fy, wy, x1, x2, field, ws, op1, op2):
    odd_x, odd_z = flag[0] == 1, flag[2] == 1
    one, two = x1[...], x2[...]
    below, above = jnp.where(odd_x, one, two), jnp.where(odd_x, two, one)
    cells = R * EY
    field[:R] = below[:cells].reshape(R, EY, LANES)
    field[R : R + CX] = fy[...]
    field[R + CX :] = above[:cells].reshape(R, EY, LANES)
    ws[...] = jnp.zeros_like(ws)
    ws[:3] = below[cells : cells + 3]
    ws[3:6] = wy[:3]
    ws[6:9] = above[cells : cells + 3]
    turned = jnp.transpose(field[...].reshape(ROWS, LANES))
    low, high = turned[: 2 * R], turned[CZ - 2 * R :]
    op1[...] = jnp.where(odd_z, low, high)
    op2[...] = jnp.where(odd_z, high, low)


def image_pack(flag, observed, op1, op2):
    odd = flag[2] == 1
    for v in range(V):
        turned = jnp.transpose(observed[v].reshape(CX * CY, LANES))
        low, high = turned[:R], turned[CZ - R :]
        op1[v * R : (v + 1) * R, :] = jnp.where(odd, low, high)
        op2[v * R : (v + 1) * R, :] = jnp.where(odd, high, low)


def total_of(x):
    return jnp.sum(jnp.sum(x, axis=0, keepdims=True), axis=1, keepdims=True)


def split(x):
    high = x.astype(BF16)
    return high, (x - high.astype(F32)).astype(BF16)


def iota(dims, axis):
    return lax.broadcasted_iota(jnp.int32, dims, axis)


def pick(taps, v, d, offset, scale):
    got = jnp.zeros(offset.shape, F32)
    for k in range(K):
        got = jnp.where(offset == k, taps[v, d, k], got)
    return got * scale


def inverse_sum(taps, v, d):
    total = taps[v, d, 0]
    for k in range(1, K):
        total = total + taps[v, d, k]
    return 1.0 / jnp.full((8, LANES), total, F32)[:1]


def bands(taps, by, byt, wz1, wz2, tz1, tz2, tz3, tx):
    for v in range(V):
        rows = slice(v * CY, (v + 1) * CY)
        scale = inverse_sum(taps, v, 0) * inverse_sum(taps, v, 1)
        column = iota((CY, LANES), 1)
        got = pick(taps, v, 1, column % EY - iota((CY, LANES), 0), scale)
        high, low = split(got)
        by[rows, :] = jnp.where(column < 2 * EY, high.astype(F32), low.astype(F32)).astype(BF16)

    def turned_y(v, got):
        lane = iota((EY, LANES), 1)
        scale = inverse_sum(taps, v, 0) * inverse_sum(taps, v, 1)
        here = pick(taps, v, 1, iota((EY, LANES), 0) - lane % CY, scale)
        return jnp.where(lane // CY == v, here, got)

    both = lax.fori_loop(0, V, turned_y, jnp.zeros((EY, LANES), F32))
    high, low = split(both)
    byt[:EY, :] = high.astype(F32)
    byt[EY:, :] = low.astype(F32)

    owner = iota((8, LANES), 1) // (2 * R)
    for k in range(K):
        row = jnp.zeros((8, LANES), F32)
        for v in range(V):
            row = jnp.where(owner == v, taps[v, 0, k], row)
        tx[k : k + 1, :] = row[:1]
    tx[K:, :] = jnp.zeros((24 - K, LANES), F32)

    wz1[...] = jnp.zeros_like(wz1)
    wz2[...] = jnp.zeros_like(wz2)
    tz2[...] = jnp.zeros_like(tz2)
    tz3[...] = jnp.zeros_like(tz3)
    row, col = iota((LANES, LANES), 0), iota((LANES, LANES), 1)
    short_row, short_col = row[: 2 * R], col[: 2 * R]
    end = row[: 4 * R]
    z_end = jnp.where(end < 2 * R, end - 2 * R, end - 2 * R + CZ)
    near_row = jnp.where(short_row < R, short_row, short_row - 2 * R + CZ)
    slot_row = jnp.where(short_row < R, short_row - R, short_row - R + CZ)

    def z_of(v, carry):
        scale = inverse_sum(taps, v, 2)
        place = short_col[:1] - 2 * R * v
        z = jnp.where(place < R, place - R, place - R + CZ)
        slot_col = jnp.where((place >= 0) & (place < 2 * R), z, 4 * CZ)

        middle = pick(taps, v, 2, row - col + R, scale)
        high, low = split(middle)
        wz1[v, :LANES, :LANES] = high
        wz1[v, LANES:, :LANES] = high
        wz2[v, :LANES, :LANES] = low
        high, low = split(jnp.transpose(middle))
        tz1[v, :LANES, :] = high
        tz1[v, LANES:, :] = high
        tz2[v, :LANES, :] = low

        near = pick(taps, v, 2, near_row - slot_col + R, scale)
        zeros = jnp.zeros((R, LANES), F32)
        for at, piece in (
            (0, jnp.concatenate([near[:R], zeros], axis=0)),
            (LANES - 2 * R, jnp.concatenate([zeros, near[R:]], axis=0)),
        ):
            high, low = split(piece)
            wz1[v, at : at + 2 * R, LANES:] = high
            wz1[v, LANES + at : LANES + at + 2 * R, LANES:] = high
            wz2[v, at : at + 2 * R, LANES:] = low

        for half, z_out in ((slice(0, LANES), col[:1]), (slice(LANES, 2 * LANES), slot_col)):
            high, low = split(pick(taps, v, 2, z_end - z_out + R, scale))
            wz2[v, LANES : LANES + 4 * R, half] = high
            wz2[v, LANES + 4 * R : LANES + 8 * R, half] = high
            wz2[v, LANES + 8 * R : LANES + 12 * R, half] = low

        high, low = split(pick(taps, v, 2, short_col - slot_row + R, scale))
        first = pl.multiple_of(v * 2 * R, 2 * R)
        tz2[v, pl.ds(LANES + first, 2 * R), :] = high
        tz3[v, pl.ds(first, 2 * R), :] = low
        tz3[v, pl.ds(LANES + first, 2 * R), :] = high
        return carry

    lax.fori_loop(0, V, z_of, 0)


BANDS = ((0, 8), (8, 24), (24, 32))


def main_kernel(
    flag, taps, cover, field, w9, z1, z2, i1, i2, observed, by, byt, wz1, wz2, tz1, tz2, tz3, tx,
    mid, op1, op2, sums,
    et, image_e, gs, hs, hp, xs, xe, pe, ys, wy, part,
):
    odd_x, odd_z = flag[0] == 1, flag[2] == 1
    one, two = z1[...], z2[...]
    below, above = jnp.where(odd_z, one, two), jnp.where(odd_z, two, one)
    e = jnp.concatenate([below, above], axis=0)
    et[...] = jnp.transpose(
        jnp.concatenate([e, e, e, jnp.zeros((LANES - 12 * R, ROWS), F32)], axis=0)
    )
    one, two = i1[...], i2[...]
    below, above = jnp.where(odd_z, one, two), jnp.where(odd_z, two, one)
    rows_e = []
    for v in range(V):
        rows_e += [below[v * R : (v + 1) * R], above[v * R : (v + 1) * R]]
    image_e[...] = jnp.transpose(jnp.concatenate(rows_e, axis=0)).reshape(CX, CY, LANES)

    for bx in range(3):
        for j in range(3):
            w_row = w9[bx * 3 + j : bx * 3 + j + 1, :]
            for q in range(BANDS[j][0], BANDS[j][1], 8):
                rows = slice(q, q + 8)
                high = w_row * byt[q : q + 8]
                wy[bx, rows, :LANES] = high
                wy[bx, rows, LANES : 2 * LANES] = high
                wy[bx, rows, 2 * LANES :] = w_row * byt[EY + q : EY + q + 8]

    face = iota((LANES, LANES), 1)
    face_low = (face >= 4 * R) & (face < 8 * R)
    lhs = by[:, : 3 * EY]
    for x in range(EX):
        high, low = split(field[x])
        e_high, e_low = split(et[x * EY : (x + 1) * EY, :])
        top = jnp.concatenate([high, e_high], axis=1)
        rhs = jnp.concatenate([top, jnp.concatenate([low, e_low], axis=1), top], axis=0)
        got = jnp.dot(lhs, rhs, preferred_element_type=F32)
        high, low = split(got[:, :LANES])
        gs[:, x, :, :LANES] = high.reshape(V, CY, LANES)
        gs[:, x, :, LANES : 2 * LANES] = low.reshape(V, CY, LANES)
        e_got = got[:, LANES:]
        e_high = e_got.astype(BF16).astype(F32)
        both = jnp.where(face_low, e_got - e_high, e_high).astype(BF16)
        gs[:, x, :, 2 * LANES :] = both.reshape(V, CY, LANES)

    for v in range(V):
        block = gs[v].reshape(EX * CY, 3 * LANES)
        got = jnp.dot(block[:, : 2 * LANES], wz1[v], preferred_element_type=F32)
        second = jnp.concatenate([block[:, :LANES], block[:, 2 * LANES :]], axis=1)
        got += jnp.dot(second, wz2[v], preferred_element_type=F32)
        hs[v] = got[:, :LANES].reshape(EX, CY, LANES)
        ends = got[:, LANES:].reshape(EX, CY, LANES)
        if v == 0:
            hp[...] = ends
        else:
            hp[...] += ends

    for b in range(0, CY, 8):
        rows = slice(b, b + 8)
        for a in range(CX):
            acc = tx[0:1, :] * hp[a, rows]
            for k in range(1, K):
                acc += tx[k : k + 1, :] * hp[a + k, rows]
            xe[a, rows] = image_e[a, rows] / acc
    for i in range(EX):
        acc = None
        for a in range(max(0, i - K + 1), min(CX, i + 1)):
            term = tx[i - a : i - a + 1, :] * xe[a]
            acc = term if acc is None else acc + term
        high, low = split(acc)
        pe[i, :, :LANES] = high
        pe[i, :, LANES:] = low

    lane = iota((8, LANES), 1)
    seen = jnp.zeros((8, LANES), F32)
    packed = pe[...].reshape(EX * CY, 2 * LANES)
    for v in range(V):
        t = [taps[v, 0, k] for k in range(K)]
        own = cover[v].astype(F32)
        for b in range(0, CY, 8):
            rows = slice(b, b + 8)
            for a in range(CX):
                acc = t[0] * hs[v, a, rows]
                for k in range(1, K):
                    acc += t[k] * hs[v, a + k, rows]
                image = observed[v, a, rows]
                seen = seen + own * image
                xs[v, a, rows] = image / acc
        for i in range(EX):
            acc = None
            for a in range(max(0, i - K + 1), min(CX, i + 1)):
                term = t[i - a] * xs[v, a]
                acc = term if acc is None else acc + term
            high, low = split(acc)
            gs[v, i, :, :LANES] = high
            gs[v, i, :, LANES : 2 * LANES] = low
        block = gs[v].reshape(EX * CY, 3 * LANES)
        got = jnp.dot(block[:, : 2 * LANES], tz1[v], preferred_element_type=F32)
        second = jnp.concatenate([block[:, :LANES], packed[:, :LANES]], axis=1)
        got += jnp.dot(second, tz2[v], preferred_element_type=F32)
        got += jnp.dot(packed, tz3[v], preferred_element_type=F32)
        for q, piece in enumerate(split(got)):
            piece = piece.reshape(EX // 2, 2, CY, LANES)
            rows = slice((q * V + v) * CY, (q * V + v + 1) * CY)
            ys[:, rows, :LANES] = piece[:, 0]
            ys[:, rows, LANES:] = piece[:, 1]

    for x in range(0, EX, 2):
        bx = 0 if x < R else (1 if x < R + CX else 2)
        got = jnp.dot(
            wy[bx, :, : 2 * LANES].astype(BF16), ys[x // 2], preferred_element_type=F32
        )
        got += jnp.dot(
            wy[bx, :, 2 * LANES :].astype(BF16), ys[x // 2, : V * CY], preferred_element_type=F32
        )
        part[x] = got[:, :LANES]
        part[x + 1] = got[:, LANES:]

    mid[...] = part[R : R + CX]
    for i in range(R):
        low, high = part[i], part[R + CX + i]
        op1[i * EY : (i + 1) * EY, :] = jnp.where(odd_x, low, high)
        op2[i * EY : (i + 1) * EY, :] = jnp.where(odd_x, high, low)

    def count_of(at):
        row = w9[at : at + 1, :]
        return jnp.maximum(jnp.sum(row, axis=1, keepdims=True) * (1.0 / CY), 1.0)

    total = jnp.zeros((8, LANES), F32)
    for bx in range(3):
        x0, x1 = BANDS[bx]
        for j in range(3):
            y0, y1 = BANDS[j]
            block = (field[x0:x1, y0:y1] * part[x0:x1, y0:y1]).reshape((-1, 8, LANES))
            total += jnp.sum(block, axis=0) / count_of(bx * 3 + j)
    target = seen / count_of(4)
    both = jnp.where(lane < 64, total_of(target), total_of(total))[:4]
    for p in range(sums.shape[0]):
        sums[p] = both


def x_add(flag, part, r1, r2, mid, op1, op2):
    odd_x, odd_y = flag[0] == 1, flag[1] == 1
    for a in range(CX):
        rows = slice((a % R) * EY, (a % R + 1) * EY)
        one, two = r1[rows, :], r2[rows, :]
        plane = part[a] + (jnp.where(odd_x, one, two) if a < R else jnp.where(odd_x, two, one))
        mid[a] = plane[R : R + CY]
        low, high = plane[:R], plane[R + CY :]
        op1[a * R : (a + 1) * R, :] = jnp.where(odd_y, low, high)
        op2[a * R : (a + 1) * R, :] = jnp.where(odd_y, high, low)


def y_add(flag, cover, part, r1, r2, est, sums, out):
    odd = flag[1] == 1
    gathered = jnp.sum(sums[...], axis=0)[:1]
    lane = iota((1, LANES), 1)
    target = jnp.sum(jnp.where(lane == 0, gathered, 0.0), axis=1, keepdims=True)
    total = jnp.sum(jnp.where(lane == 64, gathered, 0.0), axis=1, keepdims=True)
    count = jnp.sum(spread_cover(cover)[:1], axis=1, keepdims=True) * (1.0 / CY)
    by = jnp.broadcast_to(target / total / count, (8, LANES))
    for a in range(CX):
        one, two = r1[a * R : (a + 1) * R, :], r2[a * R : (a + 1) * R, :]
        out[a, :R] = est[a, :R] * (part[a, :R] + jnp.where(odd, one, two)) * by
        out[a, R:] = est[a, R:] * (part[a, R:] + jnp.where(odd, two, one)) * by


def on_device(estimate, observed, coverage, psf_taps):
    flag = jnp.stack([lax.axis_index(axis) % 2 for axis in ALL]).astype(jnp.int32)
    cover = coverage.reshape(V)
    peers = lax.axis_size(ALL)

    op = shape(R * CX + 8, LANES)
    y1, y2 = kernel_call(
        y_pack,
        (op, op),
        scratch=(
            pltpu.SMEM((V,), jnp.int32),
            pltpu.VMEM((CX, CY, CZ), F32),
            pltpu.SemaphoreType.DMA((2,)),
        ),
        n_in=3,
        in_smem=1,
        in_hbm=2,
        mib=60,
    )(flag, cover, estimate)
    y1, y2 = swap(y1, y2, "by")
    op = shape(V * R, CX * CY)
    i1, i2 = kernel_call(image_pack, (op, op), n_in=2, in_smem=1, flops=10**7)(flag, observed)
    i1, i2 = swap(i1, i2, "bz")
    square = shape(V, 2 * LANES, LANES, dtype=BF16)
    wide = shape(V, 2 * LANES, 2 * LANES, dtype=BF16)
    tables = kernel_call(
        bands,
        (
            shape(V * CY, LANES, dtype=BF16),
            shape(2 * EY, LANES),
            wide,
            wide,
            square,
            square,
            square,
            shape(24, LANES),
        ),
        n_in=1,
        in_smem=1,
        flops=2 * 10**8,
    )(psf_taps)
    op = shape(EY * R + 8, LANES)
    fy, wy, x1, x2 = kernel_call(
        x_pack, (shape(CX, EY, LANES), shape(8, LANES), op, op), n_in=5, in_smem=2
    )(flag, cover, estimate, y1, y2)
    x1, x2 = swap(x1, x2, "bx")
    op = shape(2 * R, ROWS)
    field, w9, z1, z2 = kernel_call(
        z_pack, (shape(EX, EY, LANES), shape(16, LANES), op, op), n_in=5, in_smem=1
    )(flag, fy, wy, x1, x2)
    z1, z2 = swap(z1, z2, "bz")

    op = shape(EY * R, LANES)
    part, x1, x2, sums = kernel_call(
        main_kernel,
        (shape(CX, EY, LANES), op, op, shape(peers, 4, LANES)),
        scratch=(
            pltpu.VMEM((ROWS, LANES), F32),
            pltpu.VMEM((CX, CY, LANES), F32),
            pltpu.VMEM((V, EX, CY, 3 * LANES), BF16),
            pltpu.VMEM((V, EX, CY, LANES), F32),
            pltpu.VMEM((EX, CY, LANES), F32),
            pltpu.VMEM((V, CX, CY, LANES), F32),
            pltpu.VMEM((CX, CY, LANES), F32),
            pltpu.VMEM((EX, CY, 2 * LANES), BF16),
            pltpu.VMEM((EX // 2, 2 * V * CY, 2 * LANES), BF16),
            pltpu.VMEM((3, EY, 3 * LANES), F32),
            pltpu.VMEM((EX, EY, LANES), F32),
        ),
        n_in=18,
        in_smem=3,
        mib=30,
        flops=2 * 10**9,
    )(flag, psf_taps, cover, field, w9, z1, z2, i1, i2, observed, *tables)

    x1, x2 = swap(x1, x2, "bx")
    sums = lax.all_to_all(sums, ALL, 0, 0)
    op = shape(R * CX, LANES)
    part, y1, y2 = kernel_call(x_add, (shape(CX, CY, LANES), op, op), n_in=4, in_smem=1)(
        flag, part, x1, x2
    )
    y1, y2 = swap(y1, y2, "by")
    return kernel_call(y_add, shape(CX, CY, LANES), n_in=7, in_smem=2)(
        flag, cover, part, y1, y2, estimate, sums
    )


def solution(mesh):
    spec = P("bx", "by", "bz")
    views_spec = P(None, "bx", "by", "bz")

    return jax.shard_map(
        on_device,
        mesh=mesh,
        in_specs=(spec, views_spec, views_spec, P()),
        out_specs=spec,
        check_vma=False,
    )
```

```python
import jax
import jax.numpy as jnp
from jax import lax
from jax.experimental import pallas as pl
from jax.experimental.pallas import tpu as pltpu
from jax.sharding import PartitionSpec as P


ALL = ("bx", "by", "bz")
F32, BF16 = jnp.float32, jnp.bfloat16
V, R, K = 8, 8, 17
CX, CY, CZ = 16, 16, 128
EX, EY = CX + 2 * R, CY + 2 * R
ROWS = EX * EY
LANES = 128


def pairs(count, first):
    both = []
    for i in range(first, count - 1, 2):
        both += [(i, i + 1), (i + 1, i)]
    return both


def swap(one, two, axis):
    count = lax.axis_size(axis)
    return lax.ppermute(one, axis, pairs(count, 0)), lax.ppermute(two, axis, pairs(count, 1))


def kernel_call(body, out_shape, scratch=(), in_smem=0, flops=0, n_in=0, in_hbm=0, mib=8):
    vmem = pl.BlockSpec(memory_space=pltpu.VMEM)
    smem = pl.BlockSpec(memory_space=pltpu.SMEM)
    hbm = pl.BlockSpec(memory_space=pltpu.HBM)
    return pl.pallas_call(
        body,
        out_shape=out_shape,
        in_specs=[smem] * in_smem + [hbm] * in_hbm + [vmem] * (n_in - in_smem - in_hbm),
        out_specs=jax.tree.map(lambda _: vmem, out_shape),
        scratch_shapes=list(scratch),
        compiler_params=pltpu.CompilerParams(vmem_limit_bytes=mib * 1024 * 1024),
        cost_estimate=pl.CostEstimate(flops=flops, bytes_accessed=1024, transcendentals=0),
    )


def shape(*dims, dtype=F32):
    return jax.ShapeDtypeStruct(dims, dtype)


def is_odd(axis):
    return lax.axis_index(axis) % 2 == 1


def spread_cover(cover):
    lane = iota((8, LANES), 1) // CY
    row = jnp.zeros((8, LANES), F32)
    for v in range(V):
        row = jnp.where(lane == v, cover[v].astype(F32), row)
    return row


def y_pack(cover_hbm, est_hbm, op1, op2, w_own, cover, est, sems):
    copies = (
        pltpu.make_async_copy(est_hbm, est, sems.at[0]),
        pltpu.make_async_copy(cover_hbm, cover, sems.at[1]),
    )
    for copy in copies:
        copy.start()
    for copy in copies:
        copy.wait()
    odd = is_odd("by")
    for i in range(CX):
        low, high = est[i, :R], est[i, CY - R :]
        op1[i * R : (i + 1) * R, :] = jnp.where(odd, low, high)
        op2[i * R : (i + 1) * R, :] = jnp.where(odd, high, low)
    row = spread_cover(cover)
    op1[CX * R :, :] = row
    op2[CX * R :, :] = row
    for v in range(V):
        w_own[v : v + 1, :] = jnp.full((1, LANES), cover[v].astype(F32), F32)
    w_own[V:, :] = row


def x_pack(w_own, est, y1, y2, field, ws, op1, op2):
    odd_x, odd_y = is_odd("bx"), is_odd("by")
    one, two = y1[...], y2[...]
    below, above = jnp.where(odd_y, one, two), jnp.where(odd_y, two, one)
    cells = CX * R
    field[:, :R] = below[:cells].reshape(CX, R, LANES)
    field[:, R : R + CY] = est[...]
    field[:, R + CY :] = above[:cells].reshape(CX, R, LANES)
    ws[...] = jnp.zeros_like(ws)
    ws[:1] = below[cells : cells + 1]
    ws[1:2] = w_own[V : V + 1, :]
    ws[2:3] = above[cells : cells + 1]
    for a in range(R):
        low, high = field[a], field[CX - R + a]
        op1[a * EY : (a + 1) * EY, :] = jnp.where(odd_x, low, high)
        op2[a * EY : (a + 1) * EY, :] = jnp.where(odd_x, high, low)
    op1[R * EY :, :] = ws[...]
    op2[R * EY :, :] = ws[...]


def z_pack(fy, wy, x1, x2, field, ws, op1, op2):
    odd_x, odd_z = is_odd("bx"), is_odd("bz")
    one, two = x1[...], x2[...]
    below, above = jnp.where(odd_x, one, two), jnp.where(odd_x, two, one)
    cells = R * EY
    field[:R] = below[:cells].reshape(R, EY, LANES)
    field[R : R + CX] = fy[...]
    field[R + CX :] = above[:cells].reshape(R, EY, LANES)
    ws[...] = jnp.zeros_like(ws)
    ws[:3] = below[cells : cells + 3]
    ws[3:6] = wy[:3]
    ws[6:9] = above[cells : cells + 3]
    turned = jnp.transpose(field[...].reshape(ROWS, LANES))
    low, high = turned[: 2 * R], turned[CZ - 2 * R :]
    op1[...] = jnp.where(odd_z, low, high)
    op2[...] = jnp.where(odd_z, high, low)


def image_pack(observed, op1, op2):
    odd = is_odd("bz")
    for v in range(V):
        turned = jnp.transpose(observed[v].reshape(CX * CY, LANES))
        low, high = turned[:R], turned[CZ - R :]
        op1[v * R : (v + 1) * R, :] = jnp.where(odd, low, high)
        op2[v * R : (v + 1) * R, :] = jnp.where(odd, high, low)


def total_of(x):
    return jnp.sum(jnp.sum(x, axis=0, keepdims=True), axis=1, keepdims=True)


def split(x):
    high = x.astype(BF16)
    return high, (x - high.astype(F32)).astype(BF16)


def iota(dims, axis):
    return lax.broadcasted_iota(jnp.int32, dims, axis)


def pick(taps, v, d, offset, scale):
    got = jnp.zeros(offset.shape, F32)
    for k in range(K):
        got = jnp.where(offset == k, taps[v, d, k], got)
    return got * scale


def inverse_sum(taps, v, d):
    total = taps[v, d, 0]
    for k in range(1, K):
        total = total + taps[v, d, k]
    return 1.0 / jnp.full((8, LANES), total, F32)[:1]


def bands(taps, by, byt, wz1, wz2, tz1, tz2, tz3, tx, tap_rows):
    for v in range(V):
        rows = slice(v * CY, (v + 1) * CY)
        scale = inverse_sum(taps, v, 0) * inverse_sum(taps, v, 1)
        column = iota((CY, LANES), 1)
        got = pick(taps, v, 1, column % EY - iota((CY, LANES), 0), scale)
        high, low = split(got)
        by[rows, :] = jnp.where(column < 2 * EY, high.astype(F32), low.astype(F32)).astype(BF16)

    def turned_y(v, got):
        lane = iota((EY, LANES), 1)
        scale = inverse_sum(taps, v, 0) * inverse_sum(taps, v, 1)
        here = pick(taps, v, 1, iota((EY, LANES), 0) - lane % CY, scale)
        return jnp.where(lane // CY == v, here, got)

    both = lax.fori_loop(0, V, turned_y, jnp.zeros((EY, LANES), F32))
    high, low = split(both)
    byt[:EY, :] = high.astype(F32)
    byt[EY:, :] = low.astype(F32)

    owner = iota((8, LANES), 1) // (2 * R)
    for k in range(K):
        row = jnp.zeros((8, LANES), F32)
        for v in range(V):
            row = jnp.where(owner == v, taps[v, 0, k], row)
        tx[k : k + 1, :] = row[:1]
    tx[K:, :] = jnp.zeros((24 - K, LANES), F32)
    for v in range(V):
        for k in range(K):
            tap_rows[v, k : k + 1, :] = jnp.full((1, LANES), taps[v, 0, k], F32)

    wz1[...] = jnp.zeros_like(wz1)
    wz2[...] = jnp.zeros_like(wz2)
    tz2[...] = jnp.zeros_like(tz2)
    tz3[...] = jnp.zeros_like(tz3)
    row, col = iota((LANES, LANES), 0), iota((LANES, LANES), 1)
    short_row, short_col = row[: 2 * R], col[: 2 * R]
    end = row[: 4 * R]
    z_end = jnp.where(end < 2 * R, end - 2 * R, end - 2 * R + CZ)
    near_row = jnp.where(short_row < R, short_row, short_row - 2 * R + CZ)
    slot_row = jnp.where(short_row < R, short_row - R, short_row - R + CZ)

    def z_of(v, carry):
        scale = inverse_sum(taps, v, 2)
        place = short_col[:1] - 2 * R * v
        z = jnp.where(place < R, place - R, place - R + CZ)
        slot_col = jnp.where((place >= 0) & (place < 2 * R), z, 4 * CZ)

        middle = pick(taps, v, 2, row - col + R, scale)
        high, low = split(middle)
        wz1[v, :LANES, :LANES] = high
        wz1[v, LANES:, :LANES] = high
        wz2[v, :LANES, :LANES] = low
        high, low = split(jnp.transpose(middle))
        tz1[v, :LANES, :] = high
        tz1[v, LANES:, :] = high
        tz2[v, :LANES, :] = low

        near = pick(taps, v, 2, near_row - slot_col + R, scale)
        zeros = jnp.zeros((R, LANES), F32)
        for at, piece in (
            (0, jnp.concatenate([near[:R], zeros], axis=0)),
            (LANES - 2 * R, jnp.concatenate([zeros, near[R:]], axis=0)),
        ):
            high, low = split(piece)
            wz1[v, at : at + 2 * R, LANES:] = high
            wz1[v, LANES + at : LANES + at + 2 * R, LANES:] = high
            wz2[v, at : at + 2 * R, LANES:] = low

        for half, z_out in ((slice(0, LANES), col[:1]), (slice(LANES, 2 * LANES), slot_col)):
            high, low = split(pick(taps, v, 2, z_end - z_out + R, scale))
            wz2[v, LANES : LANES + 4 * R, half] = high
            wz2[v, LANES + 4 * R : LANES + 8 * R, half] = high
            wz2[v, LANES + 8 * R : LANES + 12 * R, half] = low

        high, low = split(pick(taps, v, 2, short_col - slot_row + R, scale))
        first = pl.multiple_of(v * 2 * R, 2 * R)
        tz2[v, pl.ds(LANES + first, 2 * R), :] = high
        tz3[v, pl.ds(first, 2 * R), :] = low
        tz3[v, pl.ds(LANES + first, 2 * R), :] = high
        return carry

    lax.fori_loop(0, V, z_of, 0)


BANDS = ((0, 8), (8, 24), (24, 32))


def main_kernel(
    field, w9, z1, z2, i1, i2, observed, w_own, by, byt, wz1, wz2, tz1, tz2, tz3, tx, tap_rows,
    mid, op1, op2, sums,
    et, image_e, gs, hs, hp, xs, xe, pe, ys, wy, part,
):
    odd_x, odd_z = is_odd("bx"), is_odd("bz")
    one, two = z1[...], z2[...]
    below, above = jnp.where(odd_z, one, two), jnp.where(odd_z, two, one)
    e = jnp.concatenate([below, above], axis=0)
    et[...] = jnp.transpose(
        jnp.concatenate([e, e, e, jnp.zeros((LANES - 12 * R, ROWS), F32)], axis=0)
    )
    one, two = i1[...], i2[...]
    below, above = jnp.where(odd_z, one, two), jnp.where(odd_z, two, one)
    rows_e = []
    for v in range(V):
        rows_e += [below[v * R : (v + 1) * R], above[v * R : (v + 1) * R]]
    image_e[...] = jnp.transpose(jnp.concatenate(rows_e, axis=0)).reshape(CX, CY, LANES)

    for bx in range(3):
        for j in range(3):
            w_row = w9[bx * 3 + j : bx * 3 + j + 1, :]
            for q in range(BANDS[j][0], BANDS[j][1], 8):
                rows = slice(q, q + 8)
                high = w_row * byt[q : q + 8]
                wy[bx, rows, :LANES] = high
                wy[bx, rows, LANES : 2 * LANES] = high
                wy[bx, rows, 2 * LANES :] = w_row * byt[EY + q : EY + q + 8]

    face = iota((LANES, LANES), 1)
    face_low = (face >= 4 * R) & (face < 8 * R)
    lhs = by[:, : 3 * EY]
    for x in range(EX):
        high, low = split(field[x])
        e_high, e_low = split(et[x * EY : (x + 1) * EY, :])
        top = jnp.concatenate([high, e_high], axis=1)
        rhs = jnp.concatenate([top, jnp.concatenate([low, e_low], axis=1), top], axis=0)
        got = jnp.dot(lhs, rhs, preferred_element_type=F32)
        high, low = split(got[:, :LANES])
        gs[:, x, :, :LANES] = high.reshape(V, CY, LANES)
        gs[:, x, :, LANES : 2 * LANES] = low.reshape(V, CY, LANES)
        e_got = got[:, LANES:]
        e_high = e_got.astype(BF16).astype(F32)
        both = jnp.where(face_low, e_got - e_high, e_high).astype(BF16)
        gs[:, x, :, 2 * LANES :] = both.reshape(V, CY, LANES)

    for v in range(V):
        block = gs[v].reshape(EX * CY, 3 * LANES)
        got = jnp.dot(block[:, : 2 * LANES], wz1[v], preferred_element_type=F32)
        second = jnp.concatenate([block[:, :LANES], block[:, 2 * LANES :]], axis=1)
        got += jnp.dot(second, wz2[v], preferred_element_type=F32)
        hs[v] = got[:, :LANES].reshape(EX, CY, LANES)
        ends = got[:, LANES:].reshape(EX, CY, LANES)
        if v == 0:
            hp[...] = ends
        else:
            hp[...] += ends

    for b in range(0, CY, 8):
        rows = slice(b, b + 8)
        for a in range(CX):
            acc = tx[0:1, :] * hp[a, rows]
            for k in range(1, K):
                acc += tx[k : k + 1, :] * hp[a + k, rows]
            xe[a, rows] = image_e[a, rows] / acc
    for i in range(EX):
        acc = None
        for a in range(max(0, i - K + 1), min(CX, i + 1)):
            term = tx[i - a : i - a + 1, :] * xe[a]
            acc = term if acc is None else acc + term
        high, low = split(acc)
        pe[i, :, :LANES] = high
        pe[i, :, LANES:] = low

    lane = iota((8, LANES), 1)
    seen = jnp.zeros((8, LANES), F32)
    packed = pe[...].reshape(EX * CY, 2 * LANES)
    for v in range(V):
        t = [tap_rows[v, k : k + 1, :] for k in range(K)]
        own = w_own[v : v + 1, :]
        for b in range(0, CY, 8):
            rows = slice(b, b + 8)
            for a in range(CX):
                acc = t[0] * hs[v, a, rows]
                for k in range(1, K):
                    acc += t[k] * hs[v, a + k, rows]
                image = observed[v, a, rows]
                seen = seen + own * image
                xs[v, a, rows] = image / acc
        for i in range(EX):
            acc = None
            for a in range(max(0, i - K + 1), min(CX, i + 1)):
                term = t[i - a] * xs[v, a]
                acc = term if acc is None else acc + term
            high, low = split(acc)
            gs[v, i, :, :LANES] = high
            gs[v, i, :, LANES : 2 * LANES] = low
        block = gs[v].reshape(EX * CY, 3 * LANES)
        got = jnp.dot(block[:, : 2 * LANES], tz1[v], preferred_element_type=F32)
        second = jnp.concatenate([block[:, :LANES], packed[:, :LANES]], axis=1)
        got += jnp.dot(second, tz2[v], preferred_element_type=F32)
        got += jnp.dot(packed, tz3[v], preferred_element_type=F32)
        for q, piece in enumerate(split(got)):
            piece = piece.reshape(EX // 2, 2, CY, LANES)
            rows = slice((q * V + v) * CY, (q * V + v + 1) * CY)
            ys[:, rows, :LANES] = piece[:, 0]
            ys[:, rows, LANES:] = piece[:, 1]

    for x in range(0, EX, 2):
        bx = 0 if x < R else (1 if x < R + CX else 2)
        got = jnp.dot(
            wy[bx, :, : 2 * LANES].astype(BF16), ys[x // 2], preferred_element_type=F32
        )
        got += jnp.dot(
            wy[bx, :, 2 * LANES :].astype(BF16), ys[x // 2, : V * CY], preferred_element_type=F32
        )
        part[x] = got[:, :LANES]
        part[x + 1] = got[:, LANES:]

    mid[...] = part[R : R + CX]
    for i in range(R):
        low, high = part[i], part[R + CX + i]
        op1[i * EY : (i + 1) * EY, :] = jnp.where(odd_x, low, high)
        op2[i * EY : (i + 1) * EY, :] = jnp.where(odd_x, high, low)

    def count_of(at):
        row = w9[at : at + 1, :]
        return jnp.maximum(jnp.sum(row, axis=1, keepdims=True) * (1.0 / CY), 1.0)

    total = jnp.zeros((8, LANES), F32)
    for bx in range(3):
        x0, x1 = BANDS[bx]
        for j in range(3):
            y0, y1 = BANDS[j]
            block = (field[x0:x1, y0:y1] * part[x0:x1, y0:y1]).reshape((-1, 8, LANES))
            total += jnp.sum(block, axis=0) / count_of(bx * 3 + j)
    target = seen / count_of(4)
    both = jnp.where(lane < 64, total_of(target), total_of(total))[:4]
    for p in range(sums.shape[0]):
        sums[p] = both


def x_add(part, r1, r2, mid, op1, op2):
    odd_x, odd_y = is_odd("bx"), is_odd("by")
    for a in range(CX):
        rows = slice((a % R) * EY, (a % R + 1) * EY)
        one, two = r1[rows, :], r2[rows, :]
        plane = part[a] + (jnp.where(odd_x, one, two) if a < R else jnp.where(odd_x, two, one))
        mid[a] = plane[R : R + CY]
        low, high = plane[:R], plane[R + CY :]
        op1[a * R : (a + 1) * R, :] = jnp.where(odd_y, low, high)
        op2[a * R : (a + 1) * R, :] = jnp.where(odd_y, high, low)


def y_add(w9, part, r1, r2, est, sums, out):
    odd = is_odd("by")
    gathered = jnp.sum(sums[...], axis=0)[:1]
    lane = iota((1, LANES), 1)
    target = jnp.sum(jnp.where(lane == 0, gathered, 0.0), axis=1, keepdims=True)
    total = jnp.sum(jnp.where(lane == 64, gathered, 0.0), axis=1, keepdims=True)
    count = jnp.sum(w9[4:5, :], axis=1, keepdims=True) * (1.0 / CY)
    by = jnp.broadcast_to(target / total / count, (8, LANES))
    for a in range(CX):
        one, two = r1[a * R : (a + 1) * R, :], r2[a * R : (a + 1) * R, :]
        out[a, :R] = est[a, :R] * (part[a, :R] + jnp.where(odd, one, two)) * by
        out[a, R:] = est[a, R:] * (part[a, R:] + jnp.where(odd, two, one)) * by


def on_device(estimate, observed, coverage, psf_taps):
    cover = coverage.reshape(V)
    peers = lax.axis_size(ALL)

    op = shape(R * CX + 8, LANES)
    y1, y2, w_own = kernel_call(
        y_pack,
        (op, op, shape(V + 8, LANES)),
        scratch=(
            pltpu.SMEM((V,), jnp.int32),
            pltpu.VMEM((CX, CY, CZ), F32),
            pltpu.SemaphoreType.DMA((2,)),
        ),
        n_in=2,
        in_hbm=2,
        mib=60,
    )(cover, estimate)
    y1, y2 = swap(y1, y2, "by")
    op = shape(V * R, CX * CY)
    i1, i2 = kernel_call(image_pack, (op, op), n_in=1, flops=10**7)(observed)
    i1, i2 = swap(i1, i2, "bz")
    square = shape(V, 2 * LANES, LANES, dtype=BF16)
    wide = shape(V, 2 * LANES, 2 * LANES, dtype=BF16)
    tables = kernel_call(
        bands,
        (
            shape(V * CY, LANES, dtype=BF16),
            shape(2 * EY, LANES),
            wide,
            wide,
            square,
            square,
            square,
            shape(24, LANES),
            shape(V, 24, LANES),
        ),
        n_in=1,
        in_smem=1,
        flops=2 * 10**8,
    )(psf_taps)
    op = shape(EY * R + 8, LANES)
    fy, wy, x1, x2 = kernel_call(
        x_pack, (shape(CX, EY, LANES), shape(8, LANES), op, op), n_in=4
    )(w_own, estimate, y1, y2)
    x1, x2 = swap(x1, x2, "bx")
    op = shape(2 * R, ROWS)
    field, w9, z1, z2 = kernel_call(
        z_pack, (shape(EX, EY, LANES), shape(16, LANES), op, op), n_in=4
    )(fy, wy, x1, x2)
    z1, z2 = swap(z1, z2, "bz")

    op = shape(EY * R, LANES)
    part, x1, x2, sums = kernel_call(
        main_kernel,
        (shape(CX, EY, LANES), op, op, shape(peers, 4, LANES)),
        scratch=(
            pltpu.VMEM((ROWS, LANES), F32),
            pltpu.VMEM((CX, CY, LANES), F32),
            pltpu.VMEM((V, EX, CY, 3 * LANES), BF16),
            pltpu.VMEM((V, EX, CY, LANES), F32),
            pltpu.VMEM((EX, CY, LANES), F32),
            pltpu.VMEM((V, CX, CY, LANES), F32),
            pltpu.VMEM((CX, CY, LANES), F32),
            pltpu.VMEM((EX, CY, 2 * LANES), BF16),
            pltpu.VMEM((EX // 2, 2 * V * CY, 2 * LANES), BF16),
            pltpu.VMEM((3, EY, 3 * LANES), F32),
            pltpu.VMEM((EX, EY, LANES), F32),
        ),
        n_in=17,
        mib=30,
        flops=2 * 10**9,
    )(field, w9, z1, z2, i1, i2, observed, w_own, *tables)

    x1, x2 = swap(x1, x2, "bx")
    sums = lax.all_to_all(sums, ALL, 0, 0)
    op = shape(R * CX, LANES)
    part, y1, y2 = kernel_call(x_add, (shape(CX, CY, LANES), op, op), n_in=3)(
        part, x1, x2
    )
    y1, y2 = swap(y1, y2, "by")
    return kernel_call(y_add, shape(CX, CY, LANES), n_in=6)(
        w9, part, y1, y2, estimate, sums
    )


def solution(mesh):
    spec = P("bx", "by", "bz")
    views_spec = P(None, "bx", "by", "bz")

    return jax.shard_map(
        on_device,
        mesh=mesh,
        in_specs=(spec, views_spec, views_spec, P()),
        out_specs=spec,
        check_vma=False,
    )
```

```python
import jax
import jax.numpy as jnp
from jax import lax
from jax.experimental import pallas as pl
from jax.experimental.pallas import tpu as pltpu
from jax.sharding import PartitionSpec as P


ALL = ("bx", "by", "bz")
F32, BF16 = jnp.float32, jnp.bfloat16
V, R, K = 8, 8, 17
CX, CY, CZ = 16, 16, 128
EX, EY = CX + 2 * R, CY + 2 * R
ROWS = EX * EY
LANES = 128


def pairs(count, first):
    both = []
    for i in range(first, count - 1, 2):
        both += [(i, i + 1), (i + 1, i)]
    return both


def swap(one, two, axis):
    count = lax.axis_size(axis)
    return lax.ppermute(one, axis, pairs(count, 0)), lax.ppermute(two, axis, pairs(count, 1))


def kernel_call(body, out_shape, scratch=(), in_smem=0, flops=0, n_in=0, in_hbm=0, mib=8):
    vmem = pl.BlockSpec(memory_space=pltpu.VMEM)
    smem = pl.BlockSpec(memory_space=pltpu.SMEM)
    hbm = pl.BlockSpec(memory_space=pltpu.HBM)
    return pl.pallas_call(
        body,
        out_shape=out_shape,
        in_specs=[smem] * in_smem + [hbm] * in_hbm + [vmem] * (n_in - in_smem - in_hbm),
        out_specs=jax.tree.map(lambda _: vmem, out_shape),
        scratch_shapes=list(scratch),
        compiler_params=pltpu.CompilerParams(vmem_limit_bytes=mib * 1024 * 1024),
        cost_estimate=pl.CostEstimate(flops=flops, bytes_accessed=1024, transcendentals=0),
    )


def shape(*dims, dtype=F32):
    return jax.ShapeDtypeStruct(dims, dtype)


def is_odd(axis):
    return lax.axis_index(axis) % 2 == 1


def spread_cover(cover):
    lane = iota((8, LANES), 1) // CY
    row = jnp.zeros((8, LANES), F32)
    for v in range(V):
        row = jnp.where(lane == v, cover[v].astype(F32), row)
    return row


def y_pack(cover_hbm, est_hbm, op1, op2, w_own, cover, est, sems):
    copies = (
        pltpu.make_async_copy(est_hbm, est, sems.at[0]),
        pltpu.make_async_copy(cover_hbm, cover, sems.at[1]),
    )
    for copy in copies:
        copy.start()
    for copy in copies:
        copy.wait()
    odd = is_odd("by")
    for i in range(CX):
        low, high = est[i, :R], est[i, CY - R :]
        op1[i * R : (i + 1) * R, :] = jnp.where(odd, low, high)
        op2[i * R : (i + 1) * R, :] = jnp.where(odd, high, low)
    row = spread_cover(cover)
    op1[CX * R :, :] = row
    op2[CX * R :, :] = row
    for v in range(V):
        w_own[v : v + 1, :] = jnp.full((1, LANES), cover[v].astype(F32), F32)
    w_own[V:, :] = row


def x_pack(w_own, est, y1, y2, field, ws, op1, op2):
    odd_x, odd_y = is_odd("bx"), is_odd("by")
    one, two = y1[...], y2[...]
    below, above = jnp.where(odd_y, one, two), jnp.where(odd_y, two, one)
    cells = CX * R
    field[:, :R] = below[:cells].reshape(CX, R, LANES)
    field[:, R : R + CY] = est[...]
    field[:, R + CY :] = above[:cells].reshape(CX, R, LANES)
    ws[...] = jnp.zeros_like(ws)
    ws[:1] = below[cells : cells + 1]
    ws[1:2] = w_own[V : V + 1, :]
    ws[2:3] = above[cells : cells + 1]
    for a in range(R):
        low, high = field[a], field[CX - R + a]
        op1[a * EY : (a + 1) * EY, :] = jnp.where(odd_x, low, high)
        op2[a * EY : (a + 1) * EY, :] = jnp.where(odd_x, high, low)
    op1[R * EY :, :] = ws[...]
    op2[R * EY :, :] = ws[...]


def z_pack(fy, wy, x1, x2, field, ws, op1, op2):
    odd_x, odd_z = is_odd("bx"), is_odd("bz")
    one, two = x1[...], x2[...]
    below, above = jnp.where(odd_x, one, two), jnp.where(odd_x, two, one)
    cells = R * EY
    field[:R] = below[:cells].reshape(R, EY, LANES)
    field[R : R + CX] = fy[...]
    field[R + CX :] = above[:cells].reshape(R, EY, LANES)
    ws[...] = jnp.zeros_like(ws)
    ws[:3] = below[cells : cells + 3]
    ws[3:6] = wy[:3]
    ws[6:9] = above[cells : cells + 3]
    turned = jnp.transpose(field[...].reshape(ROWS, LANES))
    low, high = turned[: 2 * R], turned[CZ - 2 * R :]
    op1[...] = jnp.where(odd_z, low, high)
    op2[...] = jnp.where(odd_z, high, low)


def image_pack(observed, op1, op2):
    odd = is_odd("bz")
    for v in range(V):
        turned = jnp.transpose(observed[v].reshape(CX * CY, LANES))
        low, high = turned[:R], turned[CZ - R :]
        op1[v * R : (v + 1) * R, :] = jnp.where(odd, low, high)
        op2[v * R : (v + 1) * R, :] = jnp.where(odd, high, low)


def total_of(x):
    return jnp.sum(jnp.sum(x, axis=0, keepdims=True), axis=1, keepdims=True)


def split(x):
    high = x.astype(BF16)
    return high, (x - high.astype(F32)).astype(BF16)


def iota(dims, axis):
    return lax.broadcasted_iota(jnp.int32, dims, axis)


def pick(taps, v, d, offset, scale):
    got = jnp.zeros(offset.shape, F32)
    for k in range(K):
        got = jnp.where(offset == k, taps[v, d, k], got)
    return got * scale


def inverse_sum(taps, v, d):
    total = taps[v, d, 0]
    for k in range(1, K):
        total = total + taps[v, d, k]
    return 1.0 / jnp.full((8, LANES), total, F32)[:1]


def bands(taps, by, byt, wz1, wz2):
    for v in range(V):
        rows = slice(v * CY, (v + 1) * CY)
        scale = inverse_sum(taps, v, 0) * inverse_sum(taps, v, 1)
        column = iota((CY, LANES), 1)
        got = pick(taps, v, 1, column % EY - iota((CY, LANES), 0), scale)
        high, low = split(got)
        by[rows, :] = jnp.where(column < 2 * EY, high.astype(F32), low.astype(F32)).astype(BF16)

    def turned_y(v, got):
        lane = iota((EY, LANES), 1)
        scale = inverse_sum(taps, v, 0) * inverse_sum(taps, v, 1)
        here = pick(taps, v, 1, iota((EY, LANES), 0) - lane % CY, scale)
        return jnp.where(lane // CY == v, here, got)

    both = lax.fori_loop(0, V, turned_y, jnp.zeros((EY, LANES), F32))
    high, low = split(both)
    byt[:EY, :] = high.astype(F32)
    byt[EY:, :] = low.astype(F32)

    wz1[:, :, LANES:] = jnp.zeros((V, 2 * LANES, LANES), BF16)
    wz2[:, :LANES, LANES:] = jnp.zeros((V, LANES, LANES), BF16)
    wz2[:, LANES + 12 * R :, :] = jnp.zeros((V, LANES - 12 * R, 2 * LANES), BF16)
    row, col = iota((LANES, LANES), 0), iota((LANES, LANES), 1)
    short_row = row[: 2 * R]
    end = row[: 4 * R]
    z_end = jnp.where(end < 2 * R, end - 2 * R, end - 2 * R + CZ)
    near_row = jnp.where(short_row < R, short_row, short_row - 2 * R + CZ)

    def z_of(v, carry):
        scale = inverse_sum(taps, v, 2)
        place = col[:1] - 2 * R * v
        z = jnp.where(place < R, place - R, place - R + CZ)
        slot_col = jnp.where((place >= 0) & (place < 2 * R), z, 4 * CZ)

        high, low = split(pick(taps, v, 2, row - col + R, scale))
        wz1[v, :LANES, :LANES] = high
        wz1[v, LANES:, :LANES] = high
        wz2[v, :LANES, :LANES] = low

        near = pick(taps, v, 2, near_row - slot_col + R, scale)
        zeros = jnp.zeros((R, LANES), F32)
        for at, piece in (
            (0, jnp.concatenate([near[:R], zeros], axis=0)),
            (LANES - 2 * R, jnp.concatenate([zeros, near[R:]], axis=0)),
        ):
            high, low = split(piece)
            wz1[v, at : at + 2 * R, LANES:] = high
            wz1[v, LANES + at : LANES + at + 2 * R, LANES:] = high
            wz2[v, at : at + 2 * R, LANES:] = low

        for half, z_out in ((slice(0, LANES), col[:1]), (slice(LANES, 2 * LANES), slot_col)):
            high, low = split(pick(taps, v, 2, z_end - z_out + R, scale))
            wz2[v, LANES : LANES + 4 * R, half] = high
            wz2[v, LANES + 4 * R : LANES + 8 * R, half] = high
            wz2[v, LANES + 8 * R : LANES + 12 * R, half] = low
        return carry

    lax.fori_loop(0, V, z_of, 0)


def bands_back(taps, tz1, tz2, tz3, tx, tap_rows):
    owner = iota((8, LANES), 1) // (2 * R)
    for k in range(K):
        mixed = jnp.zeros((8, LANES), F32)
        for v in range(V):
            mixed = jnp.where(owner == v, taps[v, 0, k], mixed)
            tap_rows[v, k : k + 1, :] = jnp.full((1, LANES), taps[v, 0, k], F32)
        tx[k : k + 1, :] = mixed[:1]
    tx[K:, :] = jnp.zeros((24 - K, LANES), F32)
    tz2[:, LANES:, :] = jnp.zeros((V, LANES, LANES), BF16)
    tz3[...] = jnp.zeros_like(tz3)
    row, col = iota((LANES, LANES), 0), iota((LANES, LANES), 1)
    short_row, short_col = row[: 2 * R], col[: 2 * R]
    slot_row = jnp.where(short_row < R, short_row - R, short_row - R + CZ)

    def z_of(v, carry):
        scale = inverse_sum(taps, v, 2)
        high, low = split(pick(taps, v, 2, col - row + R, scale))
        tz1[v, :LANES, :] = high
        tz1[v, LANES:, :] = high
        tz2[v, :LANES, :] = low
        high, low = split(pick(taps, v, 2, short_col - slot_row + R, scale))
        first = pl.multiple_of(v * 2 * R, 2 * R)
        tz2[v, pl.ds(LANES + first, 2 * R), :] = high
        tz3[v, pl.ds(first, 2 * R), :] = low
        tz3[v, pl.ds(LANES + first, 2 * R), :] = high
        return carry

    lax.fori_loop(0, V, z_of, 0)


BANDS = ((0, 8), (8, 24), (24, 32))


def main_kernel(
    field, w9, z1, z2, i1, i2, observed, w_own, by, byt, wz1, wz2, tz1, tz2, tz3, tx, tap_rows,
    mid, op1, op2, sums,
    et, image_e, gs, hs, hp, xs, xe, pe, ys, wy, part,
):
    odd_x, odd_z = is_odd("bx"), is_odd("bz")
    one, two = z1[...], z2[...]
    below, above = jnp.where(odd_z, one, two), jnp.where(odd_z, two, one)
    e = jnp.concatenate([below, above], axis=0)
    et[...] = jnp.transpose(
        jnp.concatenate([e, e, e, jnp.zeros((LANES - 12 * R, ROWS), F32)], axis=0)
    )
    one, two = i1[...], i2[...]
    below, above = jnp.where(odd_z, one, two), jnp.where(odd_z, two, one)
    rows_e = []
    for v in range(V):
        rows_e += [below[v * R : (v + 1) * R], above[v * R : (v + 1) * R]]
    image_e[...] = jnp.transpose(jnp.concatenate(rows_e, axis=0)).reshape(CX, CY, LANES)

    for bx in range(3):
        for j in range(3):
            w_row = w9[bx * 3 + j : bx * 3 + j + 1, :]
            for q in range(BANDS[j][0], BANDS[j][1], 8):
                rows = slice(q, q + 8)
                high = w_row * byt[q : q + 8]
                wy[bx, rows, :LANES] = high
                wy[bx, rows, LANES : 2 * LANES] = high
                wy[bx, rows, 2 * LANES :] = w_row * byt[EY + q : EY + q + 8]

    face = iota((LANES, LANES), 1)
    face_low = (face >= 4 * R) & (face < 8 * R)
    lhs = by[:, : 3 * EY]
    for x in range(EX):
        high, low = split(field[x])
        e_high, e_low = split(et[x * EY : (x + 1) * EY, :])
        top = jnp.concatenate([high, e_high], axis=1)
        rhs = jnp.concatenate([top, jnp.concatenate([low, e_low], axis=1), top], axis=0)
        got = jnp.dot(lhs, rhs, preferred_element_type=F32)
        high, low = split(got[:, :LANES])
        gs[:, x, :, :LANES] = high.reshape(V, CY, LANES)
        gs[:, x, :, LANES : 2 * LANES] = low.reshape(V, CY, LANES)
        e_got = got[:, LANES:]
        e_high = e_got.astype(BF16).astype(F32)
        both = jnp.where(face_low, e_got - e_high, e_high).astype(BF16)
        gs[:, x, :, 2 * LANES :] = both.reshape(V, CY, LANES)

    for v in range(V):
        block = gs[v].reshape(EX * CY, 3 * LANES)
        got = jnp.dot(block[:, : 2 * LANES], wz1[v], preferred_element_type=F32)
        second = jnp.concatenate([block[:, :LANES], block[:, 2 * LANES :]], axis=1)
        got += jnp.dot(second, wz2[v], preferred_element_type=F32)
        hs[v] = got[:, :LANES].reshape(EX, CY, LANES)
        ends = got[:, LANES:].reshape(EX, CY, LANES)
        if v == 0:
            hp[...] = ends
        else:
            hp[...] += ends

    for b in range(0, CY, 8):
        rows = slice(b, b + 8)
        for a in range(CX):
            acc = tx[0:1, :] * hp[a, rows]
            for k in range(1, K):
                acc += tx[k : k + 1, :] * hp[a + k, rows]
            xe[a, rows] = image_e[a, rows] / acc
    for i in range(EX):
        acc = None
        for a in range(max(0, i - K + 1), min(CX, i + 1)):
            term = tx[i - a : i - a + 1, :] * xe[a]
            acc = term if acc is None else acc + term
        high, low = split(acc)
        pe[i, :, :LANES] = high
        pe[i, :, LANES:] = low

    lane = iota((8, LANES), 1)
    seen = jnp.zeros((8, LANES), F32)
    packed = pe[...].reshape(EX * CY, 2 * LANES)
    for v in range(V):
        t = [tap_rows[v, k : k + 1, :] for k in range(K)]
        own = w_own[v : v + 1, :]
        for b in range(0, CY, 8):
            rows = slice(b, b + 8)
            for a in range(CX):
                acc = t[0] * hs[v, a, rows]
                for k in range(1, K):
                    acc += t[k] * hs[v, a + k, rows]
                image = observed[v, a, rows]
                seen = seen + own * image
                xs[v, a, rows] = image / acc
        for i in range(EX):
            acc = None
            for a in range(max(0, i - K + 1), min(CX, i + 1)):
                term = t[i - a] * xs[v, a]
                acc = term if acc is None else acc + term
            high, low = split(acc)
            gs[v, i, :, :LANES] = high
            gs[v, i, :, LANES : 2 * LANES] = low
        block = gs[v].reshape(EX * CY, 3 * LANES)
        got = jnp.dot(block[:, : 2 * LANES], tz1[v], preferred_element_type=F32)
        second = jnp.concatenate([block[:, :LANES], packed[:, :LANES]], axis=1)
        got += jnp.dot(second, tz2[v], preferred_element_type=F32)
        got += jnp.dot(packed, tz3[v], preferred_element_type=F32)
        for q, piece in enumerate(split(got)):
            piece = piece.reshape(EX // 2, 2, CY, LANES)
            rows = slice((q * V + v) * CY, (q * V + v + 1) * CY)
            ys[:, rows, :LANES] = piece[:, 0]
            ys[:, rows, LANES:] = piece[:, 1]

    for x in range(0, EX, 2):
        bx = 0 if x < R else (1 if x < R + CX else 2)
        got = jnp.dot(
            wy[bx, :, : 2 * LANES].astype(BF16), ys[x // 2], preferred_element_type=F32
        )
        got += jnp.dot(
            wy[bx, :, 2 * LANES :].astype(BF16), ys[x // 2, : V * CY], preferred_element_type=F32
        )
        part[x] = got[:, :LANES]
        part[x + 1] = got[:, LANES:]

    mid[...] = part[R : R + CX]
    for i in range(R):
        low, high = part[i], part[R + CX + i]
        op1[i * EY : (i + 1) * EY, :] = jnp.where(odd_x, low, high)
        op2[i * EY : (i + 1) * EY, :] = jnp.where(odd_x, high, low)

    def count_of(at):
        row = w9[at : at + 1, :]
        return jnp.maximum(jnp.sum(row, axis=1, keepdims=True) * (1.0 / CY), 1.0)

    total = jnp.zeros((8, LANES), F32)
    for bx in range(3):
        x0, x1 = BANDS[bx]
        for j in range(3):
            y0, y1 = BANDS[j]
            block = (field[x0:x1, y0:y1] * part[x0:x1, y0:y1]).reshape((-1, 8, LANES))
            total += jnp.sum(block, axis=0) / count_of(bx * 3 + j)
    target = seen / count_of(4)
    both = jnp.where(lane < 64, total_of(target), total_of(total))[:4]
    for p in range(sums.shape[0]):
        sums[p] = both


def x_add(part, r1, r2, mid, op1, op2):
    odd_x, odd_y = is_odd("bx"), is_odd("by")
    for a in range(CX):
        rows = slice((a % R) * EY, (a % R + 1) * EY)
        one, two = r1[rows, :], r2[rows, :]
        plane = part[a] + (jnp.where(odd_x, one, two) if a < R else jnp.where(odd_x, two, one))
        mid[a] = plane[R : R + CY]
        low, high = plane[:R], plane[R + CY :]
        op1[a * R : (a + 1) * R, :] = jnp.where(odd_y, low, high)
        op2[a * R : (a + 1) * R, :] = jnp.where(odd_y, high, low)


def y_add(w9, part, r1, r2, est, sums, out):
    odd = is_odd("by")
    gathered = jnp.sum(sums[...], axis=0)[:1]
    lane = iota((1, LANES), 1)
    target = jnp.sum(jnp.where(lane == 0, gathered, 0.0), axis=1, keepdims=True)
    total = jnp.sum(jnp.where(lane == 64, gathered, 0.0), axis=1, keepdims=True)
    count = jnp.sum(w9[4:5, :], axis=1, keepdims=True) * (1.0 / CY)
    by = jnp.broadcast_to(target / total / count, (8, LANES))
    for a in range(CX):
        one, two = r1[a * R : (a + 1) * R, :], r2[a * R : (a + 1) * R, :]
        out[a, :R] = est[a, :R] * (part[a, :R] + jnp.where(odd, one, two)) * by
        out[a, R:] = est[a, R:] * (part[a, R:] + jnp.where(odd, two, one)) * by


def on_device(estimate, observed, coverage, psf_taps):
    cover = coverage.reshape(V)
    peers = lax.axis_size(ALL)

    op = shape(R * CX + 8, LANES)
    y1, y2, w_own = kernel_call(
        y_pack,
        (op, op, shape(V + 8, LANES)),
        scratch=(
            pltpu.SMEM((V,), jnp.int32),
            pltpu.VMEM((CX, CY, CZ), F32),
            pltpu.SemaphoreType.DMA((2,)),
        ),
        n_in=2,
        in_hbm=2,
        mib=40,
    )(cover, estimate)
    y1, y2 = swap(y1, y2, "by")
    op = shape(V * R, CX * CY)
    i1, i2 = kernel_call(image_pack, (op, op), n_in=1, flops=10**7)(observed)
    i1, i2 = swap(i1, i2, "bz")
    square = shape(V, 2 * LANES, LANES, dtype=BF16)
    wide = shape(V, 2 * LANES, 2 * LANES, dtype=BF16)
    tables = kernel_call(
        bands,
        (shape(V * CY, LANES, dtype=BF16), shape(2 * EY, LANES), wide, wide),
        n_in=1,
        in_smem=1,
        flops=10**8,
    )(psf_taps)
    turned = kernel_call(
        bands_back,
        (square, square, square, shape(24, LANES), shape(V, 24, LANES)),
        n_in=1,
        in_smem=1,
        flops=10**8,
    )(psf_taps)
    op = shape(EY * R + 8, LANES)
    fy, wy, x1, x2 = kernel_call(
        x_pack, (shape(CX, EY, LANES), shape(8, LANES), op, op), n_in=4
    )(w_own, estimate, y1, y2)
    x1, x2 = swap(x1, x2, "bx")
    op = shape(2 * R, ROWS)
    field, w9, z1, z2 = kernel_call(
        z_pack, (shape(EX, EY, LANES), shape(16, LANES), op, op), n_in=4
    )(fy, wy, x1, x2)
    z1, z2 = swap(z1, z2, "bz")

    op = shape(EY * R, LANES)
    part, x1, x2, sums = kernel_call(
        main_kernel,
        (shape(CX, EY, LANES), op, op, shape(peers, 4, LANES)),
        scratch=(
            pltpu.VMEM((ROWS, LANES), F32),
            pltpu.VMEM((CX, CY, LANES), F32),
            pltpu.VMEM((V, EX, CY, 3 * LANES), BF16),
            pltpu.VMEM((V, EX, CY, LANES), F32),
            pltpu.VMEM((EX, CY, LANES), F32),
            pltpu.VMEM((V, CX, CY, LANES), F32),
            pltpu.VMEM((CX, CY, LANES), F32),
            pltpu.VMEM((EX, CY, 2 * LANES), BF16),
            pltpu.VMEM((EX // 2, 2 * V * CY, 2 * LANES), BF16),
            pltpu.VMEM((3, EY, 3 * LANES), F32),
            pltpu.VMEM((EX, EY, LANES), F32),
        ),
        n_in=17,
        mib=30,
        flops=2 * 10**9,
    )(field, w9, z1, z2, i1, i2, observed, w_own, *tables, *turned)

    x1, x2 = swap(x1, x2, "bx")
    sums = lax.all_to_all(sums, ALL, 0, 0)
    op = shape(R * CX, LANES)
    part, y1, y2 = kernel_call(x_add, (shape(CX, CY, LANES), op, op), n_in=3)(
        part, x1, x2
    )
    y1, y2 = swap(y1, y2, "by")
    return kernel_call(y_add, shape(CX, CY, LANES), n_in=6)(
        w9, part, y1, y2, estimate, sums
    )


def solution(mesh):
    spec = P("bx", "by", "bz")
    views_spec = P(None, "bx", "by", "bz")

    return jax.shard_map(
        on_device,
        mesh=mesh,
        in_specs=(spec, views_spec, views_spec, P()),
        out_specs=spec,
        check_vma=False,
    )
```

```python
import jax
import jax.numpy as jnp
from jax import lax
from jax.experimental import pallas as pl
from jax.experimental.pallas import tpu as pltpu
from jax.sharding import PartitionSpec as P


ALL = ("bx", "by", "bz")
F32, BF16 = jnp.float32, jnp.bfloat16
V, R, K = 8, 8, 17
CX, CY, CZ = 16, 16, 128
EX, EY = CX + 2 * R, CY + 2 * R
ROWS = EX * EY
LANES = 128


def pairs(count, first):
    both = []
    for i in range(first, count - 1, 2):
        both += [(i, i + 1), (i + 1, i)]
    return both


def swap(one, two, axis):
    count = lax.axis_size(axis)
    one = lax.ppermute(one, axis, pairs(count, 0))
    two = lax.ppermute(two, axis, pairs(count, 1))
    return one, two


def kernel_call(body, out_shape, scratch=(), in_smem=0, flops=0, n_in=0, in_hbm=0, mib=8):
    vmem = pl.BlockSpec(memory_space=pltpu.VMEM)
    smem = pl.BlockSpec(memory_space=pltpu.SMEM)
    hbm = pl.BlockSpec(memory_space=pltpu.HBM)
    return pl.pallas_call(
        body,
        out_shape=out_shape,
        in_specs=[smem] * in_smem + [hbm] * in_hbm + [vmem] * (n_in - in_smem - in_hbm),
        out_specs=jax.tree.map(lambda _: vmem, out_shape),
        scratch_shapes=list(scratch),
        compiler_params=pltpu.CompilerParams(vmem_limit_bytes=mib * 1024 * 1024),
        cost_estimate=pl.CostEstimate(flops=flops, bytes_accessed=1024, transcendentals=0),
    )


def shape(*dims, dtype=F32):
    return jax.ShapeDtypeStruct(dims, dtype)


def is_odd(axis):
    return lax.axis_index(axis) % 2 == 1


def spread_cover(cover):
    lane = iota((8, LANES), 1) // CY
    row = jnp.zeros((8, LANES), F32)
    for v in range(V):
        row = jnp.where(lane == v, cover[v].astype(F32), row)
    return row


def y_pack(cover_hbm, est_hbm, op1, op2, w_own, cover, est, sems):
    copies = (
        pltpu.make_async_copy(est_hbm, est, sems.at[0]),
        pltpu.make_async_copy(cover_hbm, cover, sems.at[1]),
    )
    for copy in copies:
        copy.start()
    for copy in copies:
        copy.wait()
    odd = is_odd("by")
    for i in range(CX):
        low, high = est[i, :R], est[i, CY - R :]
        op1[i * R : (i + 1) * R, :] = jnp.where(odd, low, high)
        op2[i * R : (i + 1) * R, :] = jnp.where(odd, high, low)
    row = spread_cover(cover)
    op1[CX * R :, :] = row
    op2[CX * R :, :] = row
    for v in range(V):
        w_own[v : v + 1, :] = jnp.full((1, LANES), cover[v].astype(F32), F32)
    w_own[V:, :] = row


def x_pack(w_own, est, y1, y2, field, ws, op1, op2):
    odd_x, odd_y = is_odd("bx"), is_odd("by")
    one, two = y1[...], y2[...]
    below, above = jnp.where(odd_y, one, two), jnp.where(odd_y, two, one)
    cells = CX * R
    field[:, :R] = below[:cells].reshape(CX, R, LANES)
    field[:, R : R + CY] = est[...]
    field[:, R + CY :] = above[:cells].reshape(CX, R, LANES)
    ws[...] = jnp.zeros_like(ws)
    ws[:1] = below[cells : cells + 1]
    ws[1:2] = w_own[V : V + 1, :]
    ws[2:3] = above[cells : cells + 1]
    for a in range(R):
        low, high = field[a], field[CX - R + a]
        op1[a * EY : (a + 1) * EY, :] = jnp.where(odd_x, low, high)
        op2[a * EY : (a + 1) * EY, :] = jnp.where(odd_x, high, low)
    op1[R * EY :, :] = ws[...]
    op2[R * EY :, :] = ws[...]


def z_pack(fy, wy, x1, x2, field, ws, op1, op2):
    odd_x, odd_z = is_odd("bx"), is_odd("bz")
    one, two = x1[...], x2[...]
    below, above = jnp.where(odd_x, one, two), jnp.where(odd_x, two, one)
    cells = R * EY
    field[:R] = below[:cells].reshape(R, EY, LANES)
    field[R : R + CX] = fy[...]
    field[R + CX :] = above[:cells].reshape(R, EY, LANES)
    ws[...] = jnp.zeros_like(ws)
    ws[:3] = below[cells : cells + 3]
    ws[3:6] = wy[:3]
    ws[6:9] = above[cells : cells + 3]
    turned = jnp.transpose(field[...].reshape(ROWS, LANES))
    low, high = turned[: 2 * R], turned[CZ - 2 * R :]
    op1[...] = jnp.where(odd_z, low, high)
    op2[...] = jnp.where(odd_z, high, low)


def image_pack(observed, op1, op2):
    odd = is_odd("bz")
    for v in range(V):
        turned = jnp.transpose(observed[v].reshape(CX * CY, LANES))
        low, high = turned[:R], turned[CZ - R :]
        op1[v * R : (v + 1) * R, :] = jnp.where(odd, low, high)
        op2[v * R : (v + 1) * R, :] = jnp.where(odd, high, low)


def total_of(x):
    return jnp.sum(jnp.sum(x, axis=0, keepdims=True), axis=1, keepdims=True)


def split(x):
    high = x.astype(BF16)
    return high, (x - high.astype(F32)).astype(BF16)


def iota(dims, axis):
    return lax.broadcasted_iota(jnp.int32, dims, axis)


def pick(taps, v, d, offset, scale):
    got = jnp.zeros(offset.shape, F32)
    for k in range(K):
        got = jnp.where(offset == k, taps[v, d, k], got)
    return got * scale


def inverse_sum(taps, v, d):
    total = taps[v, d, 0]
    for k in range(1, K):
        total = total + taps[v, d, k]
    return 1.0 / jnp.full((8, LANES), total, F32)[:1]


def bands(taps, by, byt, wz1, wz2):
    for v in range(V):
        rows = slice(v * CY, (v + 1) * CY)
        scale = inverse_sum(taps, v, 0) * inverse_sum(taps, v, 1)
        column = iota((CY, LANES), 1)
        got = pick(taps, v, 1, column % EY - iota((CY, LANES), 0), scale)
        high, low = split(got)
        by[rows, :] = jnp.where(column < 2 * EY, high.astype(F32), low.astype(F32)).astype(BF16)

    def turned_y(v, got):
        lane = iota((EY, LANES), 1)
        scale = inverse_sum(taps, v, 0) * inverse_sum(taps, v, 1)
        here = pick(taps, v, 1, iota((EY, LANES), 0) - lane % CY, scale)
        return jnp.where(lane // CY == v, here, got)

    both = lax.fori_loop(0, V, turned_y, jnp.zeros((EY, LANES), F32))
    high, low = split(both)
    byt[:EY, :] = high.astype(F32)
    byt[EY:, :] = low.astype(F32)

    wz1[:, :, LANES:] = jnp.zeros((V, 2 * LANES, LANES), BF16)
    wz2[:, :LANES, LANES:] = jnp.zeros((V, LANES, LANES), BF16)
    wz2[:, LANES + 12 * R :, :] = jnp.zeros((V, LANES - 12 * R, 2 * LANES), BF16)
    row, col = iota((LANES, LANES), 0), iota((LANES, LANES), 1)
    short_row = row[: 2 * R]
    end = row[: 4 * R]
    z_end = jnp.where(end < 2 * R, end - 2 * R, end - 2 * R + CZ)
    near_row = jnp.where(short_row < R, short_row, short_row - 2 * R + CZ)

    def z_of(v, carry):
        scale = inverse_sum(taps, v, 2)
        place = col[:1] - 2 * R * v
        z = jnp.where(place < R, place - R, place - R + CZ)
        slot_col = jnp.where((place >= 0) & (place < 2 * R), z, 4 * CZ)

        high, low = split(pick(taps, v, 2, row - col + R, scale))
        wz1[v, :LANES, :LANES] = high
        wz1[v, LANES:, :LANES] = high
        wz2[v, :LANES, :LANES] = low

        near = pick(taps, v, 2, near_row - slot_col + R, scale)
        zeros = jnp.zeros((R, LANES), F32)
        for at, piece in (
            (0, jnp.concatenate([near[:R], zeros], axis=0)),
            (LANES - 2 * R, jnp.concatenate([zeros, near[R:]], axis=0)),
        ):
            high, low = split(piece)
            wz1[v, at : at + 2 * R, LANES:] = high
            wz1[v, LANES + at : LANES + at + 2 * R, LANES:] = high
            wz2[v, at : at + 2 * R, LANES:] = low

        for half, z_out in ((slice(0, LANES), col[:1]), (slice(LANES, 2 * LANES), slot_col)):
            high, low = split(pick(taps, v, 2, z_end - z_out + R, scale))
            wz2[v, LANES : LANES + 4 * R, half] = high
            wz2[v, LANES + 4 * R : LANES + 8 * R, half] = high
            wz2[v, LANES + 8 * R : LANES + 12 * R, half] = low
        return carry

    lax.fori_loop(0, V, z_of, 0)


def bands_back(taps, tz1, tz2, tz3, tx, tap_rows):
    owner = iota((8, LANES), 1) // (2 * R)
    for k in range(K):
        mixed = jnp.zeros((8, LANES), F32)
        for v in range(V):
            mixed = jnp.where(owner == v, taps[v, 0, k], mixed)
            tap_rows[v, k : k + 1, :] = jnp.full((1, LANES), taps[v, 0, k], F32)
        tx[k : k + 1, :] = mixed[:1]
    tx[K:, :] = jnp.zeros((24 - K, LANES), F32)
    tz2[:, LANES:, :] = jnp.zeros((V, LANES, LANES), BF16)
    tz3[...] = jnp.zeros_like(tz3)
    row, col = iota((LANES, LANES), 0), iota((LANES, LANES), 1)
    short_row, short_col = row[: 2 * R], col[: 2 * R]
    slot_row = jnp.where(short_row < R, short_row - R, short_row - R + CZ)

    def z_of(v, carry):
        scale = inverse_sum(taps, v, 2)
        high, low = split(pick(taps, v, 2, col - row + R, scale))
        tz1[v, :LANES, :] = high
        tz1[v, LANES:, :] = high
        tz2[v, :LANES, :] = low
        high, low = split(pick(taps, v, 2, short_col - slot_row + R, scale))
        first = pl.multiple_of(v * 2 * R, 2 * R)
        tz2[v, pl.ds(LANES + first, 2 * R), :] = high
        tz3[v, pl.ds(first, 2 * R), :] = low
        tz3[v, pl.ds(LANES + first, 2 * R), :] = high
        return carry

    lax.fori_loop(0, V, z_of, 0)


BANDS = ((0, 8), (8, 24), (24, 32))


def main_kernel(
    field, w9, z1, z2, i1, i2, observed, w_own, by, byt, wz1, wz2, tz1, tz2, tz3, tx, tap_rows,
    mid, op1, op2, sums,
    et, image_e, gs, hs, hp, xs, xe, pe, ys, wy, part,
):
    odd_x, odd_z = is_odd("bx"), is_odd("bz")
    one, two = z1[...], z2[...]
    below, above = jnp.where(odd_z, one, two), jnp.where(odd_z, two, one)
    e = jnp.concatenate([below, above], axis=0)
    et[...] = jnp.transpose(
        jnp.concatenate([e, e, e, jnp.zeros((LANES - 12 * R, ROWS), F32)], axis=0)
    )
    one, two = i1[...], i2[...]
    below, above = jnp.where(odd_z, one, two), jnp.where(odd_z, two, one)
    rows_e = []
    for v in range(V):
        rows_e += [below[v * R : (v + 1) * R], above[v * R : (v + 1) * R]]
    image_e[...] = jnp.transpose(jnp.concatenate(rows_e, axis=0)).reshape(CX, CY, LANES)

    for bx in range(3):
        for j in range(3):
            w_row = w9[bx * 3 + j : bx * 3 + j + 1, :]
            for q in range(BANDS[j][0], BANDS[j][1], 8):
                rows = slice(q, q + 8)
                high = w_row * byt[q : q + 8]
                wy[bx, rows, :LANES] = high
                wy[bx, rows, LANES : 2 * LANES] = high
                wy[bx, rows, 2 * LANES :] = w_row * byt[EY + q : EY + q + 8]

    face = iota((LANES, LANES), 1)
    face_low = (face >= 4 * R) & (face < 8 * R)
    lhs = by[:, : 3 * EY]
    for x in range(EX):
        high, low = split(field[x])
        e_high, e_low = split(et[x * EY : (x + 1) * EY, :])
        top = jnp.concatenate([high, e_high], axis=1)
        rhs = jnp.concatenate([top, jnp.concatenate([low, e_low], axis=1), top], axis=0)
        got = jnp.dot(lhs, rhs, preferred_element_type=F32)
        high, low = split(got[:, :LANES])
        gs[:, x, :, :LANES] = high.reshape(V, CY, LANES)
        gs[:, x, :, LANES : 2 * LANES] = low.reshape(V, CY, LANES)
        e_got = got[:, LANES:]
        e_high = e_got.astype(BF16).astype(F32)
        both = jnp.where(face_low, e_got - e_high, e_high).astype(BF16)
        gs[:, x, :, 2 * LANES :] = both.reshape(V, CY, LANES)

    for v in range(V):
        block = gs[v].reshape(EX * CY, 3 * LANES)
        got = jnp.dot(block[:, : 2 * LANES], wz1[v], preferred_element_type=F32)
        second = jnp.concatenate([block[:, :LANES], block[:, 2 * LANES :]], axis=1)
        got += jnp.dot(second, wz2[v], preferred_element_type=F32)
        hs[v] = got[:, :LANES].reshape(EX, CY, LANES)
        ends = got[:, LANES:].reshape(EX, CY, LANES)
        if v == 0:
            hp[...] = ends
        else:
            hp[...] += ends

    for b in range(0, CY, 8):
        rows = slice(b, b + 8)
        for a in range(CX):
            acc = tx[0:1, :] * hp[a, rows]
            for k in range(1, K):
                acc += tx[k : k + 1, :] * hp[a + k, rows]
            xe[a, rows] = image_e[a, rows] / acc
    for i in range(EX):
        acc = None
        for a in range(max(0, i - K + 1), min(CX, i + 1)):
            term = tx[i - a : i - a + 1, :] * xe[a]
            acc = term if acc is None else acc + term
        high, low = split(acc)
        pe[i, :, :LANES] = high
        pe[i, :, LANES:] = low

    lane = iota((8, LANES), 1)
    seen = jnp.zeros((8, LANES), F32)
    packed = pe[...].reshape(EX * CY, 2 * LANES)
    for v in range(V):
        t = [tap_rows[v, k : k + 1, :] for k in range(K)]
        own = w_own[v : v + 1, :]
        for b in range(0, CY, 8):
            rows = slice(b, b + 8)
            for a in range(CX):
                acc = t[0] * hs[v, a, rows]
                for k in range(1, K):
                    acc += t[k] * hs[v, a + k, rows]
                image = observed[v, a, rows]
                seen = seen + own * image
                xs[v, a, rows] = image / acc
        for i in range(EX):
            acc = None
            for a in range(max(0, i - K + 1), min(CX, i + 1)):
                term = t[i - a] * xs[v, a]
                acc = term if acc is None else acc + term
            high, low = split(acc)
            gs[v, i, :, :LANES] = high
            gs[v, i, :, LANES : 2 * LANES] = low
        block = gs[v].reshape(EX * CY, 3 * LANES)
        got = jnp.dot(block[:, : 2 * LANES], tz1[v], preferred_element_type=F32)
        second = jnp.concatenate([block[:, :LANES], packed[:, :LANES]], axis=1)
        got += jnp.dot(second, tz2[v], preferred_element_type=F32)
        got += jnp.dot(packed, tz3[v], preferred_element_type=F32)
        for q, piece in enumerate(split(got)):
            piece = piece.reshape(EX // 2, 2, CY, LANES)
            rows = slice((q * V + v) * CY, (q * V + v + 1) * CY)
            ys[:, rows, :LANES] = piece[:, 0]
            ys[:, rows, LANES:] = piece[:, 1]

    for x in range(0, EX, 2):
        bx = 0 if x < R else (1 if x < R + CX else 2)
        got = jnp.dot(
            wy[bx, :, : 2 * LANES].astype(BF16), ys[x // 2], preferred_element_type=F32
        )
        got += jnp.dot(
            wy[bx, :, 2 * LANES :].astype(BF16), ys[x // 2, : V * CY], preferred_element_type=F32
        )
        part[x] = got[:, :LANES]
        part[x + 1] = got[:, LANES:]

    mid[...] = part[R : R + CX]
    for i in range(R):
        low, high = part[i], part[R + CX + i]
        op1[i * EY : (i + 1) * EY, :] = jnp.where(odd_x, low, high)
        op2[i * EY : (i + 1) * EY, :] = jnp.where(odd_x, high, low)

    def count_of(at):
        row = w9[at : at + 1, :]
        return jnp.maximum(jnp.sum(row, axis=1, keepdims=True) * (1.0 / CY), 1.0)

    total = jnp.zeros((8, LANES), F32)
    for bx in range(3):
        x0, x1 = BANDS[bx]
        for j in range(3):
            y0, y1 = BANDS[j]
            block = (field[x0:x1, y0:y1] * part[x0:x1, y0:y1]).reshape((-1, 8, LANES))
            total += jnp.sum(block, axis=0) / count_of(bx * 3 + j)
    target = seen / count_of(4)
    both = jnp.where(lane < 64, total_of(target), total_of(total))[:4]
    for p in range(sums.shape[0]):
        sums[p] = both


def x_add(part, r1, r2, mid, op1, op2):
    odd_x, odd_y = is_odd("bx"), is_odd("by")
    for a in range(CX):
        rows = slice((a % R) * EY, (a % R + 1) * EY)
        one, two = r1[rows, :], r2[rows, :]
        plane = part[a] + (jnp.where(odd_x, one, two) if a < R else jnp.where(odd_x, two, one))
        mid[a] = plane[R : R + CY]
        low, high = plane[:R], plane[R + CY :]
        op1[a * R : (a + 1) * R, :] = jnp.where(odd_y, low, high)
        op2[a * R : (a + 1) * R, :] = jnp.where(odd_y, high, low)


def y_add(w9, part, r1, r2, est, sums, out):
    odd = is_odd("by")
    gathered = jnp.sum(sums[...], axis=0)[:1]
    lane = iota((1, LANES), 1)
    target = jnp.sum(jnp.where(lane == 0, gathered, 0.0), axis=1, keepdims=True)
    total = jnp.sum(jnp.where(lane == 64, gathered, 0.0), axis=1, keepdims=True)
    count = jnp.sum(w9[4:5, :], axis=1, keepdims=True) * (1.0 / CY)
    by = jnp.broadcast_to(target / total / count, (8, LANES))
    for a in range(CX):
        one, two = r1[a * R : (a + 1) * R, :], r2[a * R : (a + 1) * R, :]
        out[a, :R] = est[a, :R] * (part[a, :R] + jnp.where(odd, one, two)) * by
        out[a, R:] = est[a, R:] * (part[a, R:] + jnp.where(odd, two, one)) * by


def on_device(estimate, observed, coverage, psf_taps):
    cover = coverage.reshape(V)
    peers = lax.axis_size(ALL)

    op = shape(R * CX + 8, LANES)
    y1, y2, w_own = kernel_call(
        y_pack,
        (op, op, shape(V + 8, LANES)),
        scratch=(
            pltpu.SMEM((V,), jnp.int32),
            pltpu.VMEM((CX, CY, CZ), F32),
            pltpu.SemaphoreType.DMA((2,)),
        ),
        n_in=2,
        in_hbm=2,
        mib=60,
    )(cover, estimate)
    y1, y2 = swap(y1, y2, "by")
    op = shape(V * R, CX * CY)
    i1, i2 = kernel_call(image_pack, (op, op), n_in=1, flops=10**7)(observed)
    i1, i2 = swap(i1, i2, "bz")
    square = shape(V, 2 * LANES, LANES, dtype=BF16)
    wide = shape(V, 2 * LANES, 2 * LANES, dtype=BF16)
    tables = kernel_call(
        bands,
        (shape(V * CY, LANES, dtype=BF16), shape(2 * EY, LANES), wide, wide),
        n_in=1,
        in_smem=1,
        flops=10**8,
    )(psf_taps)
    turned = kernel_call(
        bands_back,
        (square, square, square, shape(24, LANES), shape(V, 24, LANES)),
        n_in=1,
        in_smem=1,
        flops=10**8,
    )(psf_taps)
    op = shape(EY * R + 8, LANES)
    fy, wy, x1, x2 = kernel_call(
        x_pack, (shape(CX, EY, LANES), shape(8, LANES), op, op), n_in=4
    )(w_own, estimate, y1, y2)
    x1, x2 = swap(x1, x2, "bx")
    op = shape(2 * R, ROWS)
    field, w9, z1, z2 = kernel_call(
        z_pack, (shape(EX, EY, LANES), shape(16, LANES), op, op), n_in=4
    )(fy, wy, x1, x2)
    z1, z2 = swap(z1, z2, "bz")

    op = shape(EY * R, LANES)
    part, x1, x2, sums = kernel_call(
        main_kernel,
        (shape(CX, EY, LANES), op, op, shape(peers, 4, LANES)),
        scratch=(
            pltpu.VMEM((ROWS, LANES), F32),
            pltpu.VMEM((CX, CY, LANES), F32),
            pltpu.VMEM((V, EX, CY, 3 * LANES), BF16),
            pltpu.VMEM((V, EX, CY, LANES), F32),
            pltpu.VMEM((EX, CY, LANES), F32),
            pltpu.VMEM((V, CX, CY, LANES), F32),
            pltpu.VMEM((CX, CY, LANES), F32),
            pltpu.VMEM((EX, CY, 2 * LANES), BF16),
            pltpu.VMEM((EX // 2, 2 * V * CY, 2 * LANES), BF16),
            pltpu.VMEM((3, EY, 3 * LANES), F32),
            pltpu.VMEM((EX, EY, LANES), F32),
        ),
        n_in=17,
        mib=30,
        flops=2 * 10**9,
    )(field, w9, z1, z2, i1, i2, observed, w_own, *tables, *turned)

    x1, x2 = swap(x1, x2, "bx")
    sums = lax.all_to_all(sums, ALL, 0, 0)
    op = shape(R * CX, LANES)
    part, y1, y2 = kernel_call(x_add, (shape(CX, CY, LANES), op, op), n_in=3)(
        part, x1, x2
    )
    y1, y2 = swap(y1, y2, "by")
    return kernel_call(y_add, shape(CX, CY, LANES), n_in=6)(
        w9, part, y1, y2, estimate, sums
    )


def solution(mesh):
    spec = P("bx", "by", "bz")
    views_spec = P(None, "bx", "by", "bz")

    return jax.shard_map(
        on_device,
        mesh=mesh,
        in_specs=(spec, views_spec, views_spec, P()),
        out_specs=spec,
        check_vma=False,
    )
```
